32 devices in a mesh: rep: 4 (over x, y), dp: 8 (over z, core).
Axes of the slice: x: 2, y: 2, z: 4, core: 2. Of those that a mesh axis runs over, the one named last changes fastest.
Arguments:
- g_w_gate: bfloat16 [32, 2, 1024, 3200], P(('rep', 'dp')), parts along dimension 0
- g_w_up: bfloat16 [32, 2, 1024, 3200], P(('rep', 'dp')), parts along dimension 0
- g_w_down: bfloat16 [32, 2, 3200, 1024], P(('rep', 'dp')), parts along dimension 0
- w_gate: bfloat16 [2, 1024, 3200], replicated
- w_up: bfloat16 [2, 1024, 3200], replicated
- w_down: bfloat16 [2, 3200, 1024], replicated
- m_w_gate: float32 [2, 1024, 3200], P(None, 'dp')
- m_w_up: float32 [2, 1024, 3200], P(None, 'dp')
- m_w_down: float32 [2, 3200, 1024], P(None, 'dp')
- v_w_gate: float32 [2, 1024, 3200], P(None, 'dp')
- v_w_up: float32 [2, 1024, 3200], P(None, 'dp')
- v_w_down: float32 [2, 3200, 1024], P(None, 'dp')
Outputs:
- output 1: bfloat16 [8, 1024, 3200], P('rep'), parts along dimension 0
- output 2: bfloat16 [8, 1024, 3200], P('rep'), parts along dimension 0
- output 3: bfloat16 [8, 3200, 1024], P('rep'), parts along dimension 0
- output 4: float32 [8, 1024, 3200], P('rep', 'dp'), parts along dimension 0
- output 5: float32 [8, 1024, 3200], P('rep', 'dp'), parts along dimension 0
- output 6: float32 [8, 3200, 1024], P('rep', 'dp'), parts along dimension 0
- output 7: float32 [8, 1024, 3200], P('rep', 'dp'), parts along dimension 0
- output 8: float32 [8, 1024, 3200], P('rep', 'dp'), parts along dimension 0
- output 9: float32 [8, 3200, 1024], P('rep', 'dp'), parts along dimension 0
There are 4 independent parts. The reference program is written for one: setup_inputs(seed, part) draws one part's arguments, and reference() takes and returns one part's arrays. A program takes and returns all parts, laid end to end along the dimension named above; an argument that names none is the same for every part.
All inputs are finite; a program needn't handle non-finite values.
Results may differ from the reference program's by a relative error of at most 0.022.
Values are sent between devices in bfloat16 or wider.
A program may use at most 2 GiB of HBM per device.

```python
import jax
import jax.numpy as jnp
from jax import lax

DEVICES = 8
D = 1024
FF = 3200
LAYERS = 2
NAMES = ("w_gate", "w_up", "w_down")
SHAPES = {"w_gate": (LAYERS, D, FF), "w_up": (LAYERS, D, FF), "w_down": (LAYERS, FF, D)}


def setup_inputs(seed: int = 0, part: int = 0) -> dict:
    kz, *keys = jax.random.split(jax.random.key(seed), 1 + 5 * len(NAMES))
    loud = 2.0 ** jax.random.uniform(kz, (), jnp.float32, -1.0, 1.0)
    drawn = {}
    for name, key, both in zip(NAMES, keys[:3], keys[3:6], strict=True):
        own = jax.random.normal(jax.random.fold_in(key, part), (DEVICES, *SHAPES[name]), jnp.float32)
        shared = jax.random.normal(jax.random.fold_in(both, part), SHAPES[name], jnp.float32)
        drawn["g_" + name] = (loud * (0.7 * shared / DEVICES + 0.7 * own * DEVICES**-0.5)).astype(jnp.bfloat16)
    for name, key in zip(NAMES, keys[6:9], strict=True):
        drawn[name] = (jax.random.normal(key, SHAPES[name], jnp.float32) * SHAPES[name][1] ** -0.5).astype(jnp.bfloat16)
    for name, key in zip(NAMES, keys[9:12], strict=True):
        drawn["m_" + name] = loud * 0.5 * jax.random.normal(key, SHAPES[name], jnp.float32)
    for name, key in zip(NAMES, keys[12:15], strict=True):
        drawn["v_" + name] = loud * loud * jax.random.uniform(key, SHAPES[name], jnp.float32, 0.5, 1.5)
    return drawn


def adamw(w, m, v, g):
    m = 0.9 * m + 0.1 * g
    v = 0.95 * v + 0.05 * g * g
    step = m * lax.rsqrt(v + 1e-8) + 0.1 * w
    return (w - 0.02 * step).astype(jnp.bfloat16), m, v


def clipped(gradients, sum_of_squares, count):
    factor = jnp.minimum(1.0, 0.5 * lax.rsqrt(sum_of_squares / count + 1e-30))
    return [g * factor for g in gradients]


def reference(g_w_gate, g_w_up, g_w_down, w_gate, w_up, w_down, m_w_gate, m_w_up, m_w_down, v_w_gate, v_w_up, v_w_down):
    def total(terms):
        return lax.scan(lambda so_far, term: (so_far + term.astype(jnp.float32), None), jnp.zeros(terms.shape[1:], jnp.float32), terms)[0]

    gradients = [total(terms).astype(jnp.bfloat16).astype(jnp.float32) for terms in (g_w_gate, g_w_up, g_w_down)]
    gradients = clipped(gradients, sum(jnp.sum(g * g) for g in gradients), sum(g.size for g in gradients))
    new = [
        adamw(w.astype(jnp.float32), m, v, g)
        for w, m, v, g in zip((w_gate, w_up, w_down), (m_w_gate, m_w_up, m_w_down), (v_w_gate, v_w_up, v_w_down), gradients, strict=True)
    ]
    return tuple(one[which] for which in range(3) for one in new)
```

```python
import functools

import jax
import jax.numpy as jnp
from jax import lax
from jax.experimental import pallas as pl
from jax.experimental.pallas import tpu as pltpu
from jax.sharding import PartitionSpec as P

MESH = pl.DeviceIdType.MESH
RING = 8
SLOTS = 4
LAG = 2
SHAPES = ((128, 3200, 32, 640), (128, 3200, 32, 640), (400, 1024, 80, 1024))
SUBS = tuple(r // ch for r, _, ch, _ in SHAPES)
FIRST = tuple(4 * sum(SUBS[:k]) for k in range(4))
STEPS = FIRST[3]
OWN = tuple(2 * sum(SUBS[:k]) for k in range(4))
COUNT = 19660800.0
F32, BF16 = jnp.float32, jnp.bfloat16


def pieces(k, body):
    _, cols, ch, pc = SHAPES[k]

    @pl.loop(0, ch // 16)
    def _(r):
        row = pl.multiple_of(r * 16, 16)
        for col in range(0, cols, pc):
            body(row, col)


def kernel(*refs):
    g, w, m, v = (refs[3 * i : 3 * i + 3] for i in range(4))
    out, gown, fac_out = refs[12:15], refs[15:18], refs[18]
    rest = list(refs[19:])

    def take(n):
        got, rest[:n] = tuple(rest[:n]), []
        return got

    inc, pb, wn = take(3), take(3), take(3)
    own_a, own_b, wa, wb, ma, mb, va, vb, acc_a, acc_b, stat = take(11)
    recv1, part, wr, grecv = take(3), take(3), take(3), take(3)
    own_sem, load_sem, psend, fsend, gsend, osend, isend, pwsend, pwrecv, local, stat_send, stat_recv, misc = take(13)

    rep, me = lax.axis_index("rep"), lax.axis_index("dp")
    z, c = me // 2, lax.rem(me, 2)
    dev = lambda zz, cc: (rep, 2 * zz + cc)
    partner = (rep, 2 * z + 1 - c)
    is_end = (z == 0) | (z == 3)
    left_half = z < 2
    zo = jnp.where(left_half, 0, 3)
    zm = jnp.where(left_half, 1, 2)
    zf = 3 - zm

    own = lambda k: own_a if k < 2 else own_b

    def remote(src, dst, send, recv, device):
        return pltpu.make_async_remote_copy(src_ref=src, dst_ref=dst, send_sem=send, recv_sem=recv, device_id=device, device_id_type=MESH)

    def rows(k, b, cc, s):
        r, _, ch, _ = SHAPES[k]
        step = 16
        return pl.ds(pl.multiple_of((2 * b + cc) * r + s * ch, step), SHAPES[k][2])

    def sub(k, s):
        ch = SHAPES[k][2]
        return pl.ds(pl.multiple_of(s * ch, 16), ch)

    barrier = pltpu.get_barrier_semaphore()
    for other in range(1, 8):
        pl.semaphore_signal(barrier, inc=1, device_id=(rep, lax.rem(me + other, 8)), device_id_type=MESH)
    pl.semaphore_wait(barrier, 7)

    def load(j, start):
        for k in range(3):
            @pl.when((j >= OWN[k]) & (j < OWN[k + 1]))
            def _():
                t = j - OWN[k]
                l, s, slot = t // SUBS[k], lax.rem(t, SUBS[k]), lax.rem(j, SLOTS)
                bufs = (wa, ma, va) if k < 2 else (wb, mb, vb)
                srcs = (w[k].at[l, rows(k, z, c, s)], m[k].at[l, sub(k, s)], v[k].at[l, sub(k, s)])
                for i in range(3):
                    copy = pltpu.make_async_copy(srcs[i], bufs[i].at[slot], load_sem.at[i, slot])
                    copy.start() if start else copy.wait()

    place = (z, 3 - z)
    after = (jnp.minimum(z + 1, 3), jnp.maximum(z - 1, 0))

    def where_is(f, k, i):
        t = i - FIRST[k]
        q, s = t // SUBS[k], lax.rem(t, SUBS[k])
        b = q // 2 + 2 if f == 0 else 1 - q // 2
        return b, lax.rem(q, 2), s

    def fetch(f, i):
        for k in range(3):
            @pl.when((i >= FIRST[k]) & (i < FIRST[k + 1]))
            def _():
                b, l, s = where_is(f, k, i)
                slot = lax.rem(i, RING)
                remote(g[k].at[0, l, rows(k, b, 1 - c, s)], pb[k].at[b, l, sub(k, s)], psend.at[k], part[k].at[b, l, s], partner).start()
                pltpu.make_async_copy(g[k].at[0, l, rows(k, b, c, s)], own(k).at[f, slot], own_sem.at[f, slot]).start()

    def advance(f, i):
        for k in range(3):
            @pl.when((i >= FIRST[k]) & (i < FIRST[k + 1]))
            def _():
                b, l, s = where_is(f, k, i)
                slot = lax.rem(i, RING)
                here = (b, l, sub(k, s))
                _, _, _, pc = SHAPES[k]
                acc = acc_a if k < 2 else acc_b
                pltpu.make_async_copy(g[k].at[0, l, rows(k, b, c, s)], own(k).at[f, slot], own_sem.at[f, slot]).wait()
                remote(pb[k].at[here], pb[k].at[here], psend.at[k], part[k].at[b, l, s], partner).wait_recv()
                along = remote(pb[k].at[here], inc[k].at[here], fsend.at[f, k], recv1[k].at[b, l, s], dev(after[f], c))

                def total(row, col, arrived):
                    at = (pl.ds(row, 16), pl.ds(col, pc))
                    to = (b, l, pl.ds(pl.multiple_of(s * SHAPES[k][2] + row, 16), 16), pl.ds(col, pc))
                    sum_ = own(k)[(f, slot, *at)].astype(F32) + pb[k][to].astype(F32)
                    if arrived:
                        sum_ = sum_ + inc[k][to].astype(F32)
                    return to, sum_.astype(BF16)

                @pl.when(place[f] == 0)
                def _():
                    def body(row, col):
                        to, sum_ = total(row, col, False)
                        pb[k][to] = sum_

                    pieces(k, body)

                @pl.when(place[f] > 0)
                def _():
                    along.wait_recv()

                @pl.when((place[f] > 0) & (place[f] < 3))
                def _():
                    def body(row, col):
                        to, sum_ = total(row, col, True)
                        pb[k][to] = sum_

                    pieces(k, body)

                @pl.when(place[f] < 3)
                def _():
                    along.start()

                @pl.when(place[f] == 3)
                def _():
                    def body(row, col):
                        to, sum_ = total(row, col, True)
                        inc[k][to] = sum_
                        rounded = sum_.astype(F32)
                        acc[...] += rounded * rounded

                    pieces(k, body)

    def chunks(k, body):
        @pl.loop(0, 2 * SUBS[k])
        def _(t):
            body(t // SUBS[k], lax.rem(t, SUBS[k]))

    acc_a[...] = jnp.zeros_like(acc_a)
    acc_b[...] = jnp.zeros_like(acc_b)

    @pl.loop(0, RING)
    def _(i):
        for f in range(2):
            fetch(f, i)

    @pl.loop(0, SLOTS)
    def _(j):
        load(j, True)

    @pl.loop(0, STEPS + 3 * LAG)
    def _(step):
        for f in range(2):
            i = step - LAG * place[f]

            @pl.when((i >= 0) & (i < STEPS))
            def _():
                advance(f, i)
                fetch(f, i + RING)

        @pl.when((step == STEPS) & is_end)
        def _():
            for k in range(3):
                def back(l, s):
                    here = inc[k].at[zm, l, sub(k, s)]
                    remote(here, here, gsend.at[k], grecv[k].at[l, s], dev(zm, c)).start()

                chunks(k, back)

    slot_of = lambda zz, cc: jnp.where(zz == 0, 0, 2) + cc

    def each_other(body):
        for other in range(1, 8):
            body(other - 1, (rep, lax.rem(me + other, 8)))

    mine = slot_of(z, c)

    @pl.when(is_end)
    def _():
        stat[mine] = jnp.full((8, 128), jnp.sum(acc_a[...]) + jnp.sum(acc_b[...]), F32)
        each_other(lambda i, d: remote(stat.at[mine], stat.at[mine], stat_send.at[i], stat_recv.at[mine], d).start())

    for source in range(4):
        @pl.when((mine != source) | jnp.logical_not(is_end))
        def _():
            remote(stat.at[source], stat.at[source], stat_send.at[0], stat_recv.at[source], partner).wait_recv()

    squares = stat[0] + stat[1] + stat[2] + stat[3]
    factor = jnp.minimum(1.0, 0.5 * lax.rsqrt(squares / COUNT + 1e-30))
    fac_out[...] = factor
    scale = factor[0:1, 0:1]

    def update(j, send):
        load(j, False)
        for k in range(3):
            @pl.when((j >= OWN[k]) & (j < OWN[k + 1]))
            def _():
                t = j - OWN[k]
                l, s, slot = t // SUBS[k], lax.rem(t, SUBS[k]), lax.rem(j, SLOTS)
                wx, mx, vx = (wa, ma, va) if k < 2 else (wb, mb, vb)
                _, _, ch, pc = SHAPES[k]

                @pl.when(jnp.logical_not(is_end))
                def _():
                    here = inc[k].at[z, l, sub(k, s)]
                    remote(here, here, gsend.at[k], grecv[k].at[l, s], partner).wait_recv()

                def body(row, col):
                    at = (slot, pl.ds(row, 16), pl.ds(col, pc))
                    to = (l, pl.ds(pl.multiple_of(s * ch + row, 16), 16), pl.ds(col, pc))
                    grad = inc[k][(z, *to)].astype(F32) * scale
                    new_m = 0.9 * mx[at] + 0.1 * grad
                    new_v = 0.95 * vx[at] + 0.05 * grad * grad
                    old = wx[at].astype(F32)
                    wn[k][to] = (old - 0.02 * (new_m * lax.rsqrt(new_v + 1e-8) + 0.1 * old)).astype(BF16)

                pieces(k, body)
                src, dst = wn[k].at[l, sub(k, s)], out[k].at[l, rows(k, z, c, s)]
                send(k, l, s, src, dst)
                remote(src, dst, pwsend.at[k], pwrecv.at[k], partner).start()
                pltpu.make_async_copy(src, dst, local.at[k]).start()
        load(j + SLOTS, True)

    def pass_on(k, l, s, b, to_sem, to):
        here = out[k].at[l, rows(k, b, c, s)]
        remote(here, here, gsend.at[k], wr[k].at[b, l, s], partner).wait_recv()
        if to is not None:
            remote(here, here, to_sem.at[k], wr[k].at[b, l, s], to).start()
        remote(here, here, pwsend.at[k], pwrecv.at[k], partner).start()

    def pass_index(j, b, to_sem, to):
        for k in range(3):
            @pl.when((j >= OWN[k]) & (j < OWN[k + 1]))
            def _():
                t = j - OWN[k]
                pass_on(k, t // SUBS[k], lax.rem(t, SUBS[k]), b, to_sem, to)

    @pl.when(is_end)
    def _():
        inward = dev(zm, c)

        @pl.loop(0, OWN[3])
        def _(j):
            update(j, lambda k, l, s, src, dst: remote(src, dst, isend.at[k], wr[k].at[z, l, s], inward).start())

        @pl.loop(0, OWN[3])
        def _(j):
            pass_index(j, zm, None, None)
            pass_index(j, zf, None, None)

        @pl.loop(0, OWN[3])
        def _(j):
            pass_index(j, 3 - zo, None, None)

    @pl.when(jnp.logical_not(is_end))
    def _():
        outward, inward = dev(zo, c), dev(zf, c)

        def both(k, l, s, src, dst):
            remote(src, dst, osend.at[k], wr[k].at[z, l, s], outward).start()
            remote(src, dst, isend.at[k], wr[k].at[z, l, s], inward).start()

        @pl.loop(0, OWN[3] + LAG)
        def _(j):
            @pl.when(j < OWN[3])
            def _():
                update(j, both)

            @pl.when(j >= LAG)
            def _():
                pass_index(j - LAG, zf, osend, outward)

        @pl.loop(0, OWN[3])
        def _(j):
            pass_index(j, zo, isend, inward)
            pass_index(j, 3 - zo, osend, outward)

    for k in range(3):
        pltpu.make_async_copy(inc[k].at[z], gown[k], misc.at[k]).start()

    for k in range(3):
        r = SHAPES[k][0]
        blocks = lambda n: pb[k].at[pl.ds(0, n)]
        sent = lambda n, sem: remote(blocks(n), blocks(n), sem, pwrecv.at[k], partner).wait_send()
        sent(4, psend.at[k])
        for f in range(2):
            @pl.when(place[f] < 3)
            def _():
                sent(2, fsend.at[f, k])

        @pl.when(is_end)
        def _():
            sent(1, gsend.at[k])
            sent(1, isend.at[k])

        @pl.when(jnp.logical_not(is_end))
        def _():
            sent(3, osend.at[k])
            sent(2, isend.at[k])

        sent(4, pwsend.at[k])
        pltpu.make_async_copy(wn[k], gown[k], local.at[k]).wait()
        half = out[k].at[:, pl.ds(0, 4 * r)]
        remote(half, half, gsend.at[k], pwrecv.at[k], partner).wait_recv()
        pltpu.make_async_copy(inc[k].at[z], gown[k], misc.at[k]).wait()

    @pl.when(is_end)
    def _():
        each_other(lambda i, d: remote(stat.at[mine], stat.at[mine], stat_send.at[i], stat_recv.at[mine], d).wait_send())


def exchange(*arrays):
    any_, dma = pl.BlockSpec(memory_space=pl.ANY), pltpu.SemaphoreType.DMA
    whole = [jax.ShapeDtypeStruct((2, 8 * r, n), BF16) for r, n, _, _ in SHAPES]
    block = [jax.ShapeDtypeStruct((2, r, n), BF16) for r, n, _, _ in SHAPES]
    (_, na, ca, pa), (_, nb, cb, pc) = SHAPES[0], SHAPES[2]
    scratch = [pltpu.VMEM((4, 2, r, n), BF16) for r, n, _, _ in SHAPES] * 2
    scratch += [pltpu.VMEM((2, r, n), BF16) for r, n, _, _ in SHAPES]
    scratch += [pltpu.VMEM((2, RING, ca, na), BF16), pltpu.VMEM((2, RING, cb, nb), BF16)]
    for dtype in (BF16, F32, F32):
        scratch += [pltpu.VMEM((SLOTS, ca, na), dtype), pltpu.VMEM((SLOTS, cb, nb), dtype)]
    scratch += [pltpu.VMEM((16, pa), F32), pltpu.VMEM((16, pc), F32), pltpu.VMEM((4, 8, 128), F32)]
    scratch += [dma((4, 2, s)) for s in SUBS] * 3 + [dma((2, s)) for s in SUBS]
    scratch += [dma((2, RING)), dma((3, SLOTS)), dma((3,)), dma((2, 3)), *[dma((3,))] * 6, dma((7,)), dma((4,)), dma((3,))]
    return pl.pallas_call(
        kernel,
        name="exchange",
        out_shape=(*whole, *block, jax.ShapeDtypeStruct((8, 128), F32)),
        in_specs=[any_] * 12,
        out_specs=(*[any_] * 6, pl.BlockSpec(memory_space=pltpu.VMEM)),
        scratch_shapes=scratch,
        compiler_params=pltpu.CompilerParams(collective_id=0, has_side_effects=True, vmem_limit_bytes=67043328),
    )(*arrays)


def solution(mesh):
    def step(*arrays):
        m, v = arrays[6:9], arrays[9:12]
        *rest, factor = exchange(*arrays)
        new, gradients = rest[:3], rest[3:]
        gradients = [g.astype(F32) * factor[0, 0] for g in gradients]
        new_m = [0.9 * one + 0.1 * g for one, g in zip(m, gradients, strict=True)]
        new_v = [0.95 * one + 0.05 * g * g for one, g in zip(v, gradients, strict=True)]
        return (*new, *new_m, *new_v)

    all_of, cut = P(None, None, None), P(None, "dp", None)
    return jax.shard_map(
        step,
        mesh=mesh,
        in_specs=(P(("rep", "dp"), None, None, None),) * 3 + (all_of,) * 3 + (cut,) * 6,
        out_specs=(P("rep", None, None),) * 3 + (P("rep", "dp", None),) * 6,
        check_vma=False,
    )
```

```python
import functools

import jax
import jax.numpy as jnp
from jax import lax
from jax.experimental import pallas as pl
from jax.experimental.pallas import tpu as pltpu
from jax.sharding import PartitionSpec as P

MESH = pl.DeviceIdType.MESH
RING = 8
SLOTS = 4
LAG = 2
PASS_LAG = 3
BEHIND = 16
SHAPES = ((128, 3200, 32, 640), (128, 3200, 32, 640), (400, 1024, 80, 1024))
SUBS = tuple(r // ch for r, _, ch, _ in SHAPES)
FIRST = (0, 4 * SUBS[0], 8 * SUBS[0], 8 * SUBS[0] + 4 * SUBS[2], 8 * SUBS[0] + 6 * SUBS[2])
STEPS = FIRST[4] + LAG
ORDER = (2, 0, 1)
OWN = {2: (0, 2 * SUBS[2]), 0: (2 * SUBS[2], 2 * (SUBS[2] + SUBS[0])), 1: (2 * (SUBS[2] + SUBS[0]), 2 * (SUBS[2] + 2 * SUBS[0]))}
BLOCK = OWN[1][1]
QUARTER = SHAPES[0][0] // 4
COUNT = 19660800.0
F32, BF16 = jnp.float32, jnp.bfloat16


def pieces(k, body):
    _, cols, ch, pc = SHAPES[k]

    @pl.loop(0, ch // 16)
    def _(r):
        row = pl.multiple_of(r * 16, 16)
        for col in range(0, cols, pc):
            body(row, col)


def kernel(*refs):
    g, w, m, v = (refs[3 * i : 3 * i + 3] for i in range(4))
    out, gown, moments, fac_out = refs[12:15], refs[15:18], refs[18:22], refs[22]
    rest = list(refs[23:])

    def take(n):
        got, rest[:n] = tuple(rest[:n]), []
        return got

    inc, pb, wn = take(3), take(3), take(3)
    inc_near, own_a, own_b, wa, wb, ma, mb, va, vb, acc_a, acc_b, stat = take(12)
    recv1, part, wr, grecv = take(3), take(3), take(3), take(2)
    near_recv, own_sem, load_sem, psend, fsend, near_send, gsend, osend, isend, pwsend, pwrecv, local = take(12)
    stat_send, stat_recv, mv_send, mv_recv, mv_fan, mv_all, misc = take(7)

    rep, me = lax.axis_index("rep"), lax.axis_index("dp")
    z, c = me // 2, lax.rem(me, 2)
    dev = lambda zz, cc: (rep, 2 * zz + cc)
    partner = (rep, 2 * z + 1 - c)
    is_end = (z == 0) | (z == 3)
    is_mid = jnp.logical_not(is_end)
    left_half = z < 2
    zo = jnp.where(left_half, 0, 3)
    zm = jnp.where(left_half, 1, 2)
    zf = 3 - zm

    own = lambda k: own_a if k < 2 else own_b

    def remote(src, dst, send, recv, device):
        return pltpu.make_async_remote_copy(src_ref=src, dst_ref=dst, send_sem=send, recv_sem=recv, device_id=device, device_id_type=MESH)

    def rows(k, b, cc, s):
        r, _, ch, _ = SHAPES[k]
        return pl.ds(pl.multiple_of((2 * b + cc) * r + s * ch, 16), ch)

    def sub(k, s):
        ch = SHAPES[k][2]
        return pl.ds(pl.multiple_of(s * ch, 16), ch)

    barrier = pltpu.get_barrier_semaphore()
    for other in range(1, 8):
        pl.semaphore_signal(barrier, inc=1, device_id=(rep, lax.rem(me + other, 8)), device_id_type=MESH)
    for other in range(1, 4):
        pl.semaphore_signal(barrier, inc=1, device_id=(lax.rem(rep + other, 4), me), device_id_type=MESH)
    pl.semaphore_wait(barrier, 10)

    def quarter(ref, which, l):
        return ref.at[l, pl.ds(pl.multiple_of(which * QUARTER, QUARTER), QUARTER)]

    held = (m[0], m[1], v[0], v[1])

    @pl.when(is_mid)
    def _():
        for i in range(4):
            for l in range(2):
                remote(quarter(held[i], rep, l), quarter(moments[i], rep, l), mv_send.at[i], mv_recv.at[i, l], dev(zo, c)).start()

    def spread(j):
        for i in range(4):
            for l in range(2):
                @pl.when(j == 2 * i + l)
                def _():
                    here = quarter(moments[i], rep, l)
                    remote(here, here, mv_send.at[i], mv_recv.at[i, l], partner).wait_recv()
                    for other in range(1, 4):
                        remote(here, here, mv_fan.at[i], mv_all.at[i], (lax.rem(rep + other, 4), me)).start()

    def load(j, b, start):
        for k in ORDER:
            @pl.when((j >= OWN[k][0]) & (j < OWN[k][1]))
            def _():
                t = j - OWN[k][0]
                l, s, slot = t // SUBS[k], lax.rem(t, SUBS[k]), lax.rem(j, SLOTS)
                bufs = (wa, ma, va) if k < 2 else (wb, mb, vb)
                m_, v_ = (m[k], v[k]) if b is z else (moments[k], moments[2 + k]) if k < 2 else (None, None)
                if m_ is None:
                    return
                srcs = (w[k].at[l, rows(k, b, c, s)], m_.at[l, sub(k, s)], v_.at[l, sub(k, s)])
                for i in range(3):
                    copy = pltpu.make_async_copy(srcs[i], bufs[i].at[slot], load_sem.at[i, slot])
                    copy.start() if start else copy.wait()

    place = (z, 3 - z)
    after = (jnp.minimum(z + 1, 3), jnp.maximum(z - 1, 0))
    middle, end, near = (2, 1), (3, 0), (1, 2)

    def where_is(f, q, i):
        k = min(q, 2)
        t = i - FIRST[q]
        u, s = t // SUBS[k], lax.rem(t, SUBS[k])
        if q < 2:
            return k, jnp.where(u < 2, middle[f], end[f]), lax.rem(u, 2), s, True
        if q == 2:
            return k, jnp.where(u < 2, end[f], middle[f]), lax.rem(u, 2), s, (u < 2) | (place[f] < 2)
        return k, near[f], u, s, place[f] < 2

    def each_part(f, i, body):
        for q in range(4):
            k, b, l, s, active = where_is(f, q, i)

            @pl.when((i >= FIRST[q]) & (i < FIRST[q + 1]) & active)
            def _():
                body(q, k, b, l, s, lax.rem(i, RING))

    def fetch(f, i):
        def start(q, k, b, l, s, slot):
            remote(g[k].at[0, l, rows(k, b, 1 - c, s)], pb[k].at[b, l, sub(k, s)], psend.at[k], part[k].at[b, l, s], partner).start()
            pltpu.make_async_copy(g[k].at[0, l, rows(k, b, c, s)], own(k).at[f, slot], own_sem.at[f, slot]).start()

        each_part(f, i, start)

    def advance(f, i):
        def step(q, k, b, l, s, slot):
            here = (b, l, sub(k, s))
            pc = SHAPES[k][3]
            acc = acc_a if k < 2 else acc_b
            pltpu.make_async_copy(g[k].at[0, l, rows(k, b, c, s)], own(k).at[f, slot], own_sem.at[f, slot]).wait()
            remote(pb[k].at[here], pb[k].at[here], psend.at[k], part[k].at[b, l, s], partner).wait_recv()
            along = remote(pb[k].at[here], inc[k].at[here], fsend.at[f, k], recv1[k].at[b, l, s], dev(after[f], c))
            aside = remote(pb[k].at[here], inc_near.at[l, sub(k, s)], near_send, near_recv.at[l, s], dev(after[f], c))

            def total(into, arrived, squares=False):
                def body(row, col):
                    at = (pl.ds(row, 16), pl.ds(col, pc))
                    down = pl.ds(pl.multiple_of(s * SHAPES[k][2] + row, 16), 16)
                    to = (b, l, down, pl.ds(col, pc))
                    sum_ = own(k)[(f, slot, *at)].astype(F32) + pb[k][to].astype(F32)
                    if "line" in arrived:
                        sum_ = sum_ + inc[k][to].astype(F32)
                    if "near" in arrived:
                        sum_ = sum_ + inc_near[(l, down, pl.ds(col, pc))].astype(F32)
                    sum_ = sum_.astype(BF16)
                    into[k][to] = sum_
                    if squares:
                        rounded = sum_.astype(F32)
                        acc[...] += rounded * rounded

                pieces(k, body)

            if q == 3:

                @pl.when(place[f] == 0)
                def _():
                    total(pb, ())
                    aside.start()

                @pl.when(place[f] == 1)
                def _():
                    along.wait_recv()
                    aside.wait_recv()
                    total(inc, ("line", "near"), True)

                return

            @pl.when(place[f] == 0)
            def _():
                total(pb, ())

            @pl.when(place[f] > 0)
            def _():
                along.wait_recv()

            @pl.when((place[f] > 0) & (place[f] < 3))
            def _():
                total(pb, ("line",))

            @pl.when(place[f] < 3)
            def _():
                along.start()

            @pl.when(place[f] == 3)
            def _():
                total(inc, ("line",), True)

        each_part(f, i, step)

    def chunks(k, body):
        @pl.loop(0, 2 * SUBS[k])
        def _(t):
            body(t // SUBS[k], lax.rem(t, SUBS[k]))

    def back(k, l, s):
        here = inc[k].at[zm, l, sub(k, s)]
        remote(here, here, gsend.at[k], grecv[k].at[l, s], dev(zm, c)).start()

    acc_a[...] = jnp.zeros_like(acc_a)
    acc_b[...] = jnp.zeros_like(acc_b)

    @pl.loop(0, RING)
    def _(i):
        for f in range(2):
            fetch(f, i)

    @pl.loop(0, SLOTS)
    def _(j):
        load(j, z, True)

    @pl.loop(0, STEPS)
    def _(step):
        for f in range(2):
            i = step - LAG * place[f] - jnp.where(place[f] == 3, BEHIND, 0)

            @pl.when((i >= 0) & (i < FIRST[4]))
            def _():
                advance(f, i)
                fetch(f, i + RING)

        @pl.when(is_end & (step >= 4) & (lax.rem(step, 2) == 0))
        def _():
            spread(step // 2 - 2)

    def each_other(body):
        for other in range(1, 8):
            body(other - 1, lax.rem(me + other, 8))

    stat[me] = jnp.full((8, 128), jnp.sum(acc_a[...]) + jnp.sum(acc_b[...]), F32)
    each_other(lambda i, d: remote(stat.at[me], stat.at[me], stat_send.at[i], stat_recv.at[me], (rep, d)).start())

    @pl.when(is_end)
    def _():
        for k in range(2):
            chunks(k, functools.partial(back, k))

    each_other(lambda i, d: remote(stat.at[d], stat.at[d], stat_send.at[0], stat_recv.at[d], partner).wait_recv())
    squares = stat[0]
    for source in range(1, 8):
        squares = squares + stat[source]
    factor = jnp.minimum(1.0, 0.5 * lax.rsqrt(squares / COUNT + 1e-30))
    fac_out[...] = factor
    scale = factor[0:1, 0:1]

    def update(j, b, send, arrays=ORDER, last=BLOCK):
        load(j, b, False)
        for k in arrays:
            @pl.when((j >= OWN[k][0]) & (j < OWN[k][1]))
            def _():
                t = j - OWN[k][0]
                l, s, slot = t // SUBS[k], lax.rem(t, SUBS[k]), lax.rem(j, SLOTS)
                wx, mx, vx = (wa, ma, va) if k < 2 else (wb, mb, vb)
                _, _, ch, pc = SHAPES[k]
                which = 0 if b is z else 1

                if k < 2:

                    @pl.when(is_mid)
                    def _():
                        here = inc[k].at[z, l, sub(k, s)]
                        remote(here, here, gsend.at[k], grecv[k].at[l, s], partner).wait_recv()

                def body(row, col):
                    at = (slot, pl.ds(row, 16), pl.ds(col, pc))
                    to = (l, pl.ds(pl.multiple_of(s * ch + row, 16), 16), pl.ds(col, pc))
                    grad = inc[k][(b, *to)].astype(F32) * scale
                    new_m = 0.9 * mx[at] + 0.1 * grad
                    new_v = 0.95 * vx[at] + 0.05 * grad * grad
                    old = wx[at].astype(F32)
                    wn[k][(which, *to)] = (old - 0.02 * (new_m * lax.rsqrt(new_v + 1e-8) + 0.1 * old)).astype(BF16)

                pieces(k, body)
                src, dst = wn[k].at[which, l, sub(k, s)], out[k].at[l, rows(k, b, c, s)]
                send(k, l, s, src, dst)
                remote(src, dst, pwsend.at[k], pwrecv.at[k], partner).start()
                pltpu.make_async_copy(src, dst, local.at[k]).start()

        @pl.when(j + SLOTS < last)
        def _():
            load(j + SLOTS, b, True)

    def pass_index(j, b, to_sem, to, along=(0, 1, 2)):
        for k in ORDER:
            @pl.when((j >= OWN[k][0]) & (j < OWN[k][1]))
            def _():
                t = j - OWN[k][0]
                l, s = t // SUBS[k], lax.rem(t, SUBS[k])
                here = out[k].at[l, rows(k, b, c, s)]
                remote(here, here, gsend.at[k], wr[k].at[b, l, s], partner).wait_recv()
                if to is not None and k in along:
                    remote(here, here, to_sem.at[k], wr[k].at[b, l, s], to).start()
                remote(here, here, pwsend.at[k], pwrecv.at[k], partner).start()

    @pl.when(is_end)
    def _():
        inward = dev(zm, c)

        @pl.loop(0, BLOCK)
        def _(j):
            update(j, z, lambda k, l, s, src, dst: remote(src, dst, isend.at[k], wr[k].at[z, l, s], inward).start())

        for i in range(4):
            three = moments[i].at[:, pl.ds(0, 3 * QUARTER)]
            remote(three, three, mv_fan.at[i], mv_all.at[i], partner).wait_recv()

        @pl.loop(OWN[0][0], OWN[0][0] + SLOTS)
        def _(j):
            load(j, zm, True)

        @pl.loop(OWN[0][0], BLOCK)
        def _(j):
            update(j, zm, lambda *_: None, (0, 1))

        @pl.loop(0, OWN[2][1])
        def _(j):
            pass_index(j, zm, None, None)
            pass_index(j, zf, None, None)

        @pl.loop(OWN[0][0], BLOCK)
        def _(j):
            pass_index(j, zf, None, None)

        @pl.loop(OWN[0][0], BLOCK)
        def _(j):
            pass_index(j, 3 - zo, None, None)

    @pl.when(is_mid)
    def _():
        outward, inward = dev(zo, c), dev(zf, c)

        def both(k, l, s, src, dst):
            if k == 2:
                remote(src, dst, osend.at[k], wr[k].at[z, l, s], outward).start()
            remote(src, dst, isend.at[k], wr[k].at[z, l, s], inward).start()

        @pl.loop(0, BLOCK + PASS_LAG)
        def _(j):
            @pl.when(j < BLOCK)
            def _():
                update(j, z, both)

            @pl.when(j >= PASS_LAG)
            def _():
                pass_index(j - PASS_LAG, zf, osend, outward)

        @pl.loop(0, BLOCK + PASS_LAG)
        def _(j):
            @pl.when(j < BLOCK)
            def _():
                pass_index(j, zo, isend, inward)

            @pl.when(j >= PASS_LAG)
            def _():
                pass_index(j - PASS_LAG, 3 - zo, osend, outward, (0, 1))

    for k in range(3):
        pltpu.make_async_copy(inc[k].at[z], gown[k], misc.at[k]).start()

    for k in range(3):
        r = SHAPES[k][0]
        blocks = lambda n: pb[k].at[pl.ds(0, n)]
        sent = lambda n, sem: remote(blocks(n), blocks(n), sem, pwrecv.at[k], partner).wait_send()
        sent(4, psend.at[k])
        for f in range(2):
            if k < 2:

                @pl.when(place[f] < 3)
                def _():
                    sent(2, fsend.at[f, k])

            else:

                @pl.when(place[f] < 2)
                def _():
                    sent(2, fsend.at[f, k])

                @pl.when(place[f] == 2)
                def _():
                    sent(1, fsend.at[f, k])

        def delivered(blocks_):
            half = out[k].at[:, pl.ds(0, blocks_ * r)]
            remote(half, half, gsend.at[k], pwrecv.at[k], partner).wait_recv()
            sent(blocks_, pwsend.at[k])

        def stored(n):
            pltpu.make_async_copy(pb[k].at[pl.ds(0, n)], pb[k].at[pl.ds(0, n)], local.at[k]).wait()

        @pl.when(is_end)
        def _():
            if k < 2:
                sent(1, gsend.at[k])
            sent(1, isend.at[k])
            delivered(4 if k < 2 else 3)
            stored(2 if k < 2 else 1)

        @pl.when(is_mid)
        def _():
            sent(2, osend.at[k])
            sent(2, isend.at[k])
            delivered(4)
            stored(1)

        pltpu.make_async_copy(inc[k].at[z], gown[k], misc.at[k]).wait()

    each_other(lambda i, d: remote(stat.at[me], stat.at[me], stat_send.at[i], stat_recv.at[me], (rep, d)).wait_send())

    @pl.when(is_end)
    def _():
        remote(inc_near, inc_near, near_send, mv_all.at[0], partner).wait_send()
        for i in range(4):
            three = moments[i].at[:, pl.ds(0, 3 * QUARTER)]
            remote(three, three, mv_fan.at[i], mv_all.at[i], partner).wait_send()

    @pl.when(is_mid)
    def _():
        for i in range(4):
            one = moments[i].at[:, pl.ds(0, QUARTER)]
            remote(one, one, mv_send.at[i], mv_all.at[i], partner).wait_send()


def exchange(*arrays):
    any_, dma = pl.BlockSpec(memory_space=pl.ANY), pltpu.SemaphoreType.DMA
    whole = [jax.ShapeDtypeStruct((2, 8 * r, n), BF16) for r, n, _, _ in SHAPES]
    block = [jax.ShapeDtypeStruct((2, r, n), BF16) for r, n, _, _ in SHAPES]
    moments = [jax.ShapeDtypeStruct((2, *SHAPES[0][:2]), F32)] * 4
    (_, na, ca, pa), (_, nb, cb, pc) = SHAPES[0], SHAPES[2]
    scratch = [pltpu.VMEM((4, 2, r, n), BF16) for r, n, _, _ in SHAPES] * 2
    scratch += [pltpu.VMEM((2 if r == SHAPES[0][0] else 1, 2, r, n), BF16) for r, n, _, _ in SHAPES]
    scratch += [pltpu.VMEM((2, *SHAPES[2][:2]), BF16)]
    scratch += [pltpu.VMEM((2, RING, ca, na), BF16), pltpu.VMEM((2, RING, cb, nb), BF16)]
    for dtype in (BF16, F32, F32):
        scratch += [pltpu.VMEM((SLOTS, ca, na), dtype), pltpu.VMEM((SLOTS, cb, nb), dtype)]
    scratch += [pltpu.VMEM((16, pa), F32), pltpu.VMEM((16, pc), F32), pltpu.VMEM((8, 8, 128), F32)]
    scratch += [dma((4, 2, s)) for s in SUBS] * 3 + [dma((2, s)) for s in SUBS[:2]]
    scratch += [dma((2, SUBS[2])), dma((2, RING)), dma((3, SLOTS)), dma((3,)), dma((2, 3)), dma, *[dma((3,))] * 6]
    scratch += [dma((7,)), dma((8,)), dma((4,)), dma((4, 2)), dma((4,)), dma((4,)), dma((3,))]
    return pl.pallas_call(
        kernel,
        name="exchange",
        out_shape=(*whole, *block, *moments, jax.ShapeDtypeStruct((8, 128), F32)),
        in_specs=[any_] * 12,
        out_specs=(*[any_] * 10, pl.BlockSpec(memory_space=pltpu.VMEM)),
        scratch_shapes=scratch,
        compiler_params=pltpu.CompilerParams(collective_id=0, has_side_effects=True, vmem_limit_bytes=67043328),
    )(*arrays)


DEPTH = 6


def fresh(arrays):
    size = [(x.shape[1] // 4, x.shape[2]) for x in arrays]

    def copy(*refs):
        n = len(arrays)
        src, dst, bufs, get, put = refs[:n], refs[n : 2 * n], refs[2 * n : 2 * n + 2], refs[-2], refs[-1]
        todo = [(k, l, p) for l in range(2) for p in range(4) for k in range(n)]
        slots, used = [], [0, 0]
        for k, _, _ in todo:
            shape = int(size[k] != size[0])
            slots.append((shape, used[shape] % DEPTH))
            used[shape] += 1

        def ends(i):
            (k, l, p), (shape, slot) = todo[i], slots[i]
            at = (l, pl.ds(p * size[k][0], size[k][0]))
            buf = bufs[shape].at[slot]
            return (
                pltpu.make_async_copy(src[k].at[at], buf, get.at[shape, slot]),
                pltpu.make_async_copy(buf, dst[k].at[at], put.at[shape, slot]),
            )

        before = [next((j for j in range(i - 1, -1, -1) if slots[j] == slots[i]), None) for i in range(len(todo))]
        unwaited = set(range(len(todo)))
        ahead = DEPTH - 2
        for i in range(-ahead, len(todo)):
            if i + ahead < len(todo):
                if before[i + ahead] is not None:
                    ends(before[i + ahead])[1].wait()
                    unwaited.discard(before[i + ahead])
                ends(i + ahead)[0].start()
            if i >= 0:
                ends(i)[0].wait()
                ends(i)[1].start()
        for i in sorted(unwaited):
            ends(i)[1].wait()

    any_ = pl.BlockSpec(memory_space=pl.ANY)
    return pl.pallas_call(
        copy,
        name="fresh",
        in_specs=[any_] * len(arrays),
        out_specs=[any_] * len(arrays),
        out_shape=[jax.ShapeDtypeStruct(x.shape, x.dtype) for x in arrays],
        scratch_shapes=[pltpu.VMEM((DEPTH, *size[0]), BF16), pltpu.VMEM((DEPTH, *size[-1]), BF16)]
        + [pltpu.SemaphoreType.DMA((2, DEPTH))] * 2,
        compiler_params=pltpu.CompilerParams(vmem_limit_bytes=2**25),
        cost_estimate=pl.CostEstimate(flops=10**8, bytes_accessed=4 * sum(x.size for x in arrays), transcendentals=0),
    )(*arrays)


def place(whole, blocks, rows, needed):
    size = blocks[0].shape

    def copy(rows_ref, needed_ref, whole_ref, *refs):
        src, dst, buf, get, put = refs[: len(blocks)], refs[len(blocks)], *refs[-3:]

        @pl.when(needed_ref[0] == 1)
        def _():
            ins = [pltpu.make_async_copy(src[i], buf.at[i], get.at[i]) for i in range(len(blocks))]
            outs = [
                pltpu.make_async_copy(buf.at[i], dst.at[:, pl.ds(pl.multiple_of(rows_ref[i], 16), size[1])], put.at[i])
                for i in range(len(blocks))
            ]
            for one in ins:
                one.start()
            for i, one in enumerate(ins):
                one.wait()
                outs[i].start()
            for one in outs:
                one.wait()

    any_, smem = pl.BlockSpec(memory_space=pl.ANY), pl.BlockSpec(memory_space=pltpu.SMEM)
    return pl.pallas_call(
        copy,
        name="place",
        in_specs=[smem, smem] + [any_] * (1 + len(blocks)),
        out_specs=any_,
        out_shape=jax.ShapeDtypeStruct(whole.shape, whole.dtype),
        scratch_shapes=[pltpu.VMEM((len(blocks), *size), whole.dtype)] + [pltpu.SemaphoreType.DMA((len(blocks),))] * 2,
        input_output_aliases={2: 0},
    )(jnp.stack(rows), needed.astype(jnp.int32)[None], whole, *blocks)


def solution(mesh):
    def step(*arrays):
        m, v = arrays[6:9], arrays[9:12]
        *rest, factor = exchange(*arrays)
        new, gradients = rest[:3], rest[3:6]

        me = lax.axis_index("dp")
        z, core = me // 2, lax.rem(me, 2)
        is_end = (z == 0) | (z == 3)
        r, cols = SHAPES[2][:2]
        far = jnp.where(z < 2, 3, 0)
        take = lambda x, cc: lax.dynamic_slice(x, (0, (2 * far + cc) * r, 0), (2, r, cols))
        mine = lax.ppermute(take(new[2], core), "dp", [(2, 0), (3, 1), (4, 6), (5, 7)])

        gradients = [g.astype(F32) * factor[0, 0] for g in gradients]
        new_m = [0.9 * one + 0.1 * g for one, g in zip(m, gradients, strict=True)]
        new_v = [0.95 * one + 0.05 * g * g for one, g in zip(v, gradients, strict=True)]
        whole = fresh(new)
        mine, whole, new_m, new_v = lax.optimization_barrier((mine, whole, new_m, new_v))

        other = lax.ppermute(mine, "dp", [(0, 1), (1, 0), (6, 7), (7, 6)])
        gate, up, down = whole
        down = place(down, (mine, other), [(2 * far + cc) * r for cc in (core, 1 - core)], is_end)
        return (gate, up, down, *new_m, *new_v)

    all_of, cut = P(None, None, None), P(None, "dp", None)
    return jax.shard_map(
        step,
        mesh=mesh,
        in_specs=(P(("rep", "dp"), None, None, None),) * 3 + (all_of,) * 3 + (cut,) * 6,
        out_specs=(P("rep", None, None),) * 3 + (P("rep", "dp", None),) * 6,
        check_vma=False,
    )
```

```python
import functools

import jax
import jax.numpy as jnp
from jax import lax
from jax.experimental import pallas as pl
from jax.experimental.pallas import tpu as pltpu
from jax.sharding import PartitionSpec as P

MESH = pl.DeviceIdType.MESH
ALL_VMEM = 67043328
RING = 8
SLOTS = 4
LAG = 2
PASS_LAG = 3
BEHIND = 16
SHAPES = ((128, 3200, 32, 640), (128, 3200, 32, 640), (400, 1024, 80, 1024))
SUBS = tuple(r // ch for r, _, ch, _ in SHAPES)
FIRST = (0, 4 * SUBS[0], 8 * SUBS[0], 8 * SUBS[0] + 4 * SUBS[2], 8 * SUBS[0] + 6 * SUBS[2])
STEPS = FIRST[4] + LAG
ORDER = (2, 0, 1)
OWN = {2: (0, 2 * SUBS[2]), 0: (2 * SUBS[2], 2 * (SUBS[2] + SUBS[0])), 1: (2 * (SUBS[2] + SUBS[0]), 2 * (SUBS[2] + 2 * SUBS[0]))}
BLOCK = OWN[1][1]
QUARTER = SHAPES[0][0] // 4
COUNT = 19660800.0
F32, BF16 = jnp.float32, jnp.bfloat16


def pieces(k, body):
    _, cols, ch, pc = SHAPES[k]

    @pl.loop(0, ch // 16)
    def _(r):
        row = pl.multiple_of(r * 16, 16)
        for col in range(0, cols, pc):
            body(row, col)


def kernel(*refs):
    g, w, m, v = (refs[3 * i : 3 * i + 3] for i in range(4))
    out, gown, moments, far, fac_out = refs[12:15], refs[15:18], refs[18:22], refs[22], refs[23]
    rest = list(refs[24:])

    def take(n):
        got, rest[:n] = tuple(rest[:n]), []
        return got

    inc, pb, wn = take(3), take(3), take(3)
    inc_near, own_a, own_b, wa, wb, ma, mb, va, vb, acc_a, acc_b, stat = take(12)
    recv1, part, wr, grecv = take(3), take(3), take(3), take(2)
    near_recv, own_sem, load_sem, psend, fsend, near_send, gsend, osend, isend, pwsend, pwrecv, local = take(12)
    stat_send, stat_recv, mv_send, mv_recv, mv_fan, mv_all, misc = take(7)

    rep, me = lax.axis_index("rep"), lax.axis_index("dp")
    z, c = me // 2, lax.rem(me, 2)
    dev = lambda zz, cc: (rep, 2 * zz + cc)
    partner = (rep, 2 * z + 1 - c)
    is_end = (z == 0) | (z == 3)
    is_mid = jnp.logical_not(is_end)
    left_half = z < 2
    zo = jnp.where(left_half, 0, 3)
    zm = jnp.where(left_half, 1, 2)
    zf = 3 - zm

    own = lambda k: own_a if k < 2 else own_b

    def remote(src, dst, send, recv, device):
        return pltpu.make_async_remote_copy(src_ref=src, dst_ref=dst, send_sem=send, recv_sem=recv, device_id=device, device_id_type=MESH)

    def rows(k, b, cc, s):
        r, _, ch, _ = SHAPES[k]
        return pl.ds(pl.multiple_of((2 * b + cc) * r + s * ch, 16), ch)

    def sub(k, s):
        ch = SHAPES[k][2]
        return pl.ds(pl.multiple_of(s * ch, 16), ch)

    barrier = pltpu.get_barrier_semaphore()
    for other in range(1, 8):
        pl.semaphore_signal(barrier, inc=1, device_id=(rep, lax.rem(me + other, 8)), device_id_type=MESH)
    for other in range(1, 4):
        pl.semaphore_signal(barrier, inc=1, device_id=(lax.rem(rep + other, 4), me), device_id_type=MESH)
    pl.semaphore_wait(barrier, 10)

    def quarter(ref, which, l):
        return ref.at[l, pl.ds(pl.multiple_of(which * QUARTER, QUARTER), QUARTER)]

    held = (m[0], m[1], v[0], v[1])

    @pl.when(is_mid)
    def _():
        for i in range(4):
            for l in range(2):
                remote(quarter(held[i], rep, l), quarter(moments[i], rep, l), mv_send.at[i], mv_recv.at[i, l], dev(zo, c)).start()

    def spread(j):
        for i in range(4):
            for l in range(2):
                @pl.when(j == 2 * i + l)
                def _():
                    here = quarter(moments[i], rep, l)
                    remote(here, here, mv_send.at[i], mv_recv.at[i, l], partner).wait_recv()
                    for other in range(1, 4):
                        remote(here, here, mv_fan.at[i], mv_all.at[i], (lax.rem(rep + other, 4), me)).start()

    def load(j, b, start):
        for k in ORDER:
            @pl.when((j >= OWN[k][0]) & (j < OWN[k][1]))
            def _():
                t = j - OWN[k][0]
                l, s, slot = t // SUBS[k], lax.rem(t, SUBS[k]), lax.rem(j, SLOTS)
                bufs = (wa, ma, va) if k < 2 else (wb, mb, vb)
                m_, v_ = (m[k], v[k]) if b is z else (moments[k], moments[2 + k]) if k < 2 else (None, None)
                if m_ is None:
                    return
                srcs = (w[k].at[l, rows(k, b, c, s)], m_.at[l, sub(k, s)], v_.at[l, sub(k, s)])
                for i in range(3):
                    copy = pltpu.make_async_copy(srcs[i], bufs[i].at[slot], load_sem.at[i, slot])
                    copy.start() if start else copy.wait()

    place = (z, 3 - z)
    after = (jnp.minimum(z + 1, 3), jnp.maximum(z - 1, 0))
    middle, end, near = (2, 1), (3, 0), (1, 2)

    def where_is(f, q, i):
        k = min(q, 2)
        t = i - FIRST[q]
        u, s = t // SUBS[k], lax.rem(t, SUBS[k])
        if q < 2:
            return k, jnp.where(u < 2, middle[f], end[f]), lax.rem(u, 2), s, True
        if q == 2:
            return k, jnp.where(u < 2, end[f], middle[f]), lax.rem(u, 2), s, (u < 2) | (place[f] < 2)
        return k, near[f], u, s, place[f] < 2

    def each_part(f, i, body):
        for q in range(4):
            k, b, l, s, active = where_is(f, q, i)

            @pl.when((i >= FIRST[q]) & (i < FIRST[q + 1]) & active)
            def _():
                body(q, k, b, l, s, lax.rem(i, RING))

    def fetch(f, i):
        def start(q, k, b, l, s, slot):
            remote(g[k].at[0, l, rows(k, b, 1 - c, s)], pb[k].at[b, l, sub(k, s)], psend.at[k], part[k].at[b, l, s], partner).start()
            pltpu.make_async_copy(g[k].at[0, l, rows(k, b, c, s)], own(k).at[f, slot], own_sem.at[f, slot]).start()

        each_part(f, i, start)

    def advance(f, i):
        def step(q, k, b, l, s, slot):
            here = (b, l, sub(k, s))
            pc = SHAPES[k][3]
            acc = acc_a if k < 2 else acc_b
            pltpu.make_async_copy(g[k].at[0, l, rows(k, b, c, s)], own(k).at[f, slot], own_sem.at[f, slot]).wait()
            remote(pb[k].at[here], pb[k].at[here], psend.at[k], part[k].at[b, l, s], partner).wait_recv()
            along = remote(pb[k].at[here], inc[k].at[here], fsend.at[f, k], recv1[k].at[b, l, s], dev(after[f], c))
            aside = remote(pb[k].at[here], inc_near.at[l, sub(k, s)], near_send, near_recv.at[l, s], dev(after[f], c))

            def total(into, arrived, squares=False):
                def body(row, col):
                    at = (pl.ds(row, 16), pl.ds(col, pc))
                    down = pl.ds(pl.multiple_of(s * SHAPES[k][2] + row, 16), 16)
                    to = (b, l, down, pl.ds(col, pc))
                    sum_ = own(k)[(f, slot, *at)].astype(F32) + pb[k][to].astype(F32)
                    if "line" in arrived:
                        sum_ = sum_ + inc[k][to].astype(F32)
                    if "near" in arrived:
                        sum_ = sum_ + inc_near[(l, down, pl.ds(col, pc))].astype(F32)
                    sum_ = sum_.astype(BF16)
                    into[k][to] = sum_
                    if squares:
                        rounded = sum_.astype(F32)
                        acc[...] += rounded * rounded

                pieces(k, body)

            if q == 3:

                @pl.when(place[f] == 0)
                def _():
                    total(pb, ())
                    aside.start()

                @pl.when(place[f] == 1)
                def _():
                    along.wait_recv()
                    aside.wait_recv()
                    total(inc, ("line", "near"), True)

                return

            @pl.when(place[f] == 0)
            def _():
                total(pb, ())

            @pl.when(place[f] > 0)
            def _():
                along.wait_recv()

            @pl.when((place[f] > 0) & (place[f] < 3))
            def _():
                total(pb, ("line",))

            @pl.when(place[f] < 3)
            def _():
                along.start()

            @pl.when(place[f] == 3)
            def _():
                total(inc, ("line",), True)

        each_part(f, i, step)

    def chunks(k, body):
        @pl.loop(0, 2 * SUBS[k])
        def _(t):
            body(t // SUBS[k], lax.rem(t, SUBS[k]))

    def back(k, l, s):
        here = inc[k].at[zm, l, sub(k, s)]
        remote(here, here, gsend.at[k], grecv[k].at[l, s], dev(zm, c)).start()

    acc_a[...] = jnp.zeros_like(acc_a)
    acc_b[...] = jnp.zeros_like(acc_b)

    @pl.loop(0, RING)
    def _(i):
        for f in range(2):
            fetch(f, i)

    @pl.loop(0, SLOTS)
    def _(j):
        load(j, z, True)

    @pl.loop(0, STEPS)
    def _(step):
        for f in range(2):
            i = step - LAG * place[f] - jnp.where(place[f] == 3, BEHIND, 0)

            @pl.when((i >= 0) & (i < FIRST[4]))
            def _():
                advance(f, i)
                fetch(f, i + RING)

        @pl.when(is_end & (step >= 4) & (lax.rem(step, 2) == 0))
        def _():
            spread(step // 2 - 2)

    def each_other(body):
        for other in range(1, 8):
            body(other - 1, lax.rem(me + other, 8))

    stat[me] = jnp.full((8, 128), jnp.sum(acc_a[...]) + jnp.sum(acc_b[...]), F32)
    each_other(lambda i, d: remote(stat.at[me], stat.at[me], stat_send.at[i], stat_recv.at[me], (rep, d)).start())

    @pl.when(is_end)
    def _():
        for k in range(2):
            chunks(k, functools.partial(back, k))

    each_other(lambda i, d: remote(stat.at[d], stat.at[d], stat_send.at[0], stat_recv.at[d], partner).wait_recv())
    squares = stat[0]
    for source in range(1, 8):
        squares = squares + stat[source]
    factor = jnp.minimum(1.0, 0.5 * lax.rsqrt(squares / COUNT + 1e-30))
    fac_out[...] = factor
    scale = factor[0:1, 0:1]

    def update(j, b, send, arrays=ORDER, last=BLOCK):
        load(j, b, False)
        for k in arrays:
            @pl.when((j >= OWN[k][0]) & (j < OWN[k][1]))
            def _():
                t = j - OWN[k][0]
                l, s, slot = t // SUBS[k], lax.rem(t, SUBS[k]), lax.rem(j, SLOTS)
                wx, mx, vx = (wa, ma, va) if k < 2 else (wb, mb, vb)
                _, _, ch, pc = SHAPES[k]
                which = 0 if b is z else 1

                if k < 2:

                    @pl.when(is_mid)
                    def _():
                        here = inc[k].at[z, l, sub(k, s)]
                        remote(here, here, gsend.at[k], grecv[k].at[l, s], partner).wait_recv()

                def body(row, col):
                    at = (slot, pl.ds(row, 16), pl.ds(col, pc))
                    to = (l, pl.ds(pl.multiple_of(s * ch + row, 16), 16), pl.ds(col, pc))
                    grad = inc[k][(b, *to)].astype(F32) * scale
                    new_m = 0.9 * mx[at] + 0.1 * grad
                    new_v = 0.95 * vx[at] + 0.05 * grad * grad
                    old = wx[at].astype(F32)
                    wn[k][(which, *to)] = (old - 0.02 * (new_m * lax.rsqrt(new_v + 1e-8) + 0.1 * old)).astype(BF16)

                pieces(k, body)
                src, dst = wn[k].at[which, l, sub(k, s)], out[k].at[l, rows(k, b, c, s)]
                send(k, l, s, src, dst)
                remote(src, dst, pwsend.at[k], pwrecv.at[k], partner).start()
                pltpu.make_async_copy(src, dst, local.at[k]).start()

        @pl.when(j + SLOTS < last)
        def _():
            load(j + SLOTS, b, True)

    def pass_index(j, b, to_sem, to, hop=None):
        for k in ORDER:
            @pl.when((j >= OWN[k][0]) & (j < OWN[k][1]))
            def _():
                t = j - OWN[k][0]
                l, s = t // SUBS[k], lax.rem(t, SUBS[k])
                there = out[k].at[l, rows(k, b, c, s)]
                aside = far.at[l, sub(k, s)] if k == 1 else None
                here = aside if k == 1 and hop == 3 else there
                remote(here, here, gsend.at[k], wr[k].at[b, l, s], partner).wait_recv()
                if to is not None and not (k == 1 and hop == 3):
                    remote(here, aside if k == 1 and hop == 2 else there, to_sem.at[k], wr[k].at[b, l, s], to).start()
                remote(here, there, pwsend.at[k], pwrecv.at[k], partner).start()

    def keep():
        for k in range(3):
            pltpu.make_async_copy(inc[k].at[z], gown[k], misc.at[k]).start()

    @pl.when(is_end)
    def _():
        inward = dev(zm, c)
        keep()

        @pl.loop(0, BLOCK)
        def _(j):
            update(j, z, lambda k, l, s, src, dst: remote(src, dst, isend.at[k], wr[k].at[z, l, s], inward).start())

        for i in range(4):
            three = moments[i].at[:, pl.ds(0, 3 * QUARTER)]
            remote(three, three, mv_fan.at[i], mv_all.at[i], partner).wait_recv()

        @pl.loop(OWN[0][0], OWN[0][0] + SLOTS)
        def _(j):
            load(j, zm, True)

        @pl.loop(OWN[0][0], BLOCK)
        def _(j):
            update(j, zm, lambda *_: None, (0, 1))

        @pl.loop(0, OWN[2][1])
        def _(j):
            pass_index(j, zm, None, None)
            pass_index(j, zf, None, None)

        @pl.loop(OWN[0][0], BLOCK)
        def _(j):
            pass_index(j, zf, None, None)

        @pl.loop(0, OWN[0][1])
        def _(j):
            pass_index(j, 3 - zo, None, None)

    @pl.when(is_mid)
    def _():
        outward, inward = dev(zo, c), dev(zf, c)

        def both(k, l, s, src, dst):
            if k == 2:
                remote(src, dst, osend.at[k], wr[k].at[z, l, s], outward).start()
            remote(src, dst, isend.at[k], wr[k].at[z, l, s], inward).start()

        @pl.loop(0, BLOCK + PASS_LAG)
        def _(j):
            @pl.when(j < BLOCK)
            def _():
                update(j, z, both)

            @pl.when(j >= PASS_LAG)
            def _():
                pass_index(j - PASS_LAG, zf, osend, outward)

        keep()

        @pl.loop(0, BLOCK + PASS_LAG)
        def _(j):
            @pl.when(j < BLOCK)
            def _():
                pass_index(j, zo, isend, inward, 2)

            @pl.when(j >= PASS_LAG)
            def _():
                pass_index(j - PASS_LAG, 3 - zo, osend, outward, 3)

    for k in range(3):
        r = SHAPES[k][0]
        blocks = lambda n: pb[k].at[pl.ds(0, n)]
        sent = lambda n, sem: remote(blocks(n), blocks(n), sem, pwrecv.at[k], partner).wait_send()
        sent(4, psend.at[k])
        for f in range(2):
            if k < 2:

                @pl.when(place[f] < 3)
                def _():
                    sent(2, fsend.at[f, k])

            else:

                @pl.when(place[f] < 2)
                def _():
                    sent(2, fsend.at[f, k])

                @pl.when(place[f] == 2)
                def _():
                    sent(1, fsend.at[f, k])

        def delivered(blocks_):
            half = out[k].at[:, pl.ds(0, blocks_ * r)]
            remote(half, half, gsend.at[k], pwrecv.at[k], partner).wait_recv()
            sent(blocks_, pwsend.at[k])

        def stored(n):
            pltpu.make_async_copy(pb[k].at[pl.ds(0, n)], pb[k].at[pl.ds(0, n)], local.at[k]).wait()

        @pl.when(is_end)
        def _():
            if k < 2:
                sent(1, gsend.at[k])
            sent(1, isend.at[k])
            delivered(3 if k == 1 else 4)
            stored(2 if k < 2 else 1)

        @pl.when(is_mid)
        def _():
            sent(1 if k == 1 else 3 if k == 2 else 2, osend.at[k])
            sent(2, isend.at[k])
            delivered(4)
            stored(1)

        pltpu.make_async_copy(inc[k].at[z], gown[k], misc.at[k]).wait()

    each_other(lambda i, d: remote(stat.at[me], stat.at[me], stat_send.at[i], stat_recv.at[me], (rep, d)).wait_send())

    @pl.when(is_end)
    def _():
        remote(inc_near, inc_near, near_send, mv_all.at[0], partner).wait_send()
        for i in range(4):
            three = moments[i].at[:, pl.ds(0, 3 * QUARTER)]
            remote(three, three, mv_fan.at[i], mv_all.at[i], partner).wait_send()

    @pl.when(is_mid)
    def _():
        for i in range(4):
            one = moments[i].at[:, pl.ds(0, QUARTER)]
            remote(one, one, mv_send.at[i], mv_all.at[i], partner).wait_send()


def exchange(*arrays):
    any_, dma = pl.BlockSpec(memory_space=pl.ANY), pltpu.SemaphoreType.DMA
    whole = [jax.ShapeDtypeStruct((2, 8 * r, n), BF16) for r, n, _, _ in SHAPES]
    block = [jax.ShapeDtypeStruct((2, r, n), BF16) for r, n, _, _ in SHAPES]
    moments = [jax.ShapeDtypeStruct((2, *SHAPES[0][:2]), F32)] * 4
    (_, na, ca, pa), (_, nb, cb, pc) = SHAPES[0], SHAPES[2]
    scratch = [pltpu.VMEM((4, 2, r, n), BF16) for r, n, _, _ in SHAPES] * 2
    scratch += [pltpu.VMEM((2 if r == SHAPES[0][0] else 1, 2, r, n), BF16) for r, n, _, _ in SHAPES]
    scratch += [pltpu.VMEM((2, *SHAPES[2][:2]), BF16)]
    scratch += [pltpu.VMEM((2, RING, ca, na), BF16), pltpu.VMEM((2, RING, cb, nb), BF16)]
    for dtype in (BF16, F32, F32):
        scratch += [pltpu.VMEM((SLOTS, ca, na), dtype), pltpu.VMEM((SLOTS, cb, nb), dtype)]
    scratch += [pltpu.VMEM((16, pa), F32), pltpu.VMEM((16, pc), F32), pltpu.VMEM((8, 8, 128), F32)]
    scratch += [dma((4, 2, s)) for s in SUBS] * 3 + [dma((2, s)) for s in SUBS[:2]]
    scratch += [dma((2, SUBS[2])), dma((2, RING)), dma((3, SLOTS)), dma((3,)), dma((2, 3)), dma, *[dma((3,))] * 6]
    scratch += [dma((7,)), dma((8,)), dma((4,)), dma((4, 2)), dma((4,)), dma((4,)), dma((3,))]
    return pl.pallas_call(
        kernel,
        name="exchange",
        out_shape=(*whole, *block, *moments, block[1], jax.ShapeDtypeStruct((8, 128), F32)),
        in_specs=[any_] * 12,
        out_specs=(*[any_] * 11, pl.BlockSpec(memory_space=pltpu.VMEM)),
        scratch_shapes=scratch,
        compiler_params=pltpu.CompilerParams(collective_id=0, has_side_effects=True, vmem_limit_bytes=ALL_VMEM),
    )(*arrays)


DEPTH = 6
MOMENT_DEPTH = 8


def finish(copies, sets, factor):
    nc, ns = len(copies), len(sets)
    size = [(x.shape[1] // 4, x.shape[2]) for x in copies]
    tall = [m.shape[1] // (4 if m.shape[1] % 64 == 0 else 5) for m, _, _ in sets]
    shapes = sorted(set(size), reverse=True)
    kinds = sorted({(t, m.shape[2]) for t, (m, _, _) in zip(tall, sets, strict=True)})
    todo = [("copy", k, l, p) for l in range(2) for p in range(4) for k in range(nc)]
    more = [("moment", k, l, p) for l in range(2) for k in range(ns) for p in range(sets[k][0].shape[1] // tall[k])]
    todo = [x for _, x in sorted([((i + 0.5) / len(todo), x) for i, x in enumerate(todo)] + [((i + 0.5) / len(more), x) for i, x in enumerate(more)])]

    def run(*refs):
        fac, refs = refs[0], list(refs[1:])

        def take(n):
            got, refs[:n] = tuple(refs[:n]), []
            return got

        src, ms, vs, gs, dst, new_m, new_v = (take(n) for n in (nc, ns, ns, ns, nc, ns, ns))
        bufs = take(len(shapes))
        mb, vb, gb = (take(len(kinds)) for _ in range(3))
        get, put = take(2) if nc else (None, None)
        mget, mput = take(2)
        scale = fac[0:1, 0:1]
        used, slots = {}, []
        for kind, k, _, _ in todo:
            shape = (kind, shapes.index(size[k]) if kind == "copy" else kinds.index((tall[k], sets[k][0].shape[2])))
            n = used.get(shape, 0)
            used[shape] = n + 1
            slots.append((*shape, n % (DEPTH if kind == "copy" else MOMENT_DEPTH)))

        def moves(i, way):
            (kind, k, l, p), (_, shape, slot) = todo[i], slots[i]
            if kind == "copy":
                at = (l, pl.ds(p * size[k][0], size[k][0]))
                buf = bufs[shape].at[slot]
                pairs = [(src[k].at[at], buf, get.at[shape, slot])] if way == 0 else [(buf, dst[k].at[at], put.at[shape, slot])]
            else:
                at = (l, pl.ds(p * tall[k], tall[k]))
                held = [x[shape].at[slot] for x in (mb, vb, gb)]
                if way == 0:
                    pairs = [(x[k].at[at], held[n], mget.at[shape, n, slot]) for n, x in enumerate((ms, vs, gs))]
                else:
                    pairs = [(held[n], x[k].at[at], mput.at[shape, n, slot]) for n, x in enumerate((new_m, new_v))]
            return [pltpu.make_async_copy(*pair) for pair in pairs]

        def start(i, way):
            for one in moves(i, way):
                one.start()

        def wait(i, way):
            for one in moves(i, way):
                one.wait()

        def compute(i):
            (kind, k, _, _), (_, shape, slot) = todo[i], slots[i]
            if kind == "copy":
                return
            wide = 640 if sets[k][0].shape[2] % 640 == 0 else 1024

            @pl.loop(0, tall[k] // 16)
            def _(r):
                for col in range(0, sets[k][0].shape[2], wide):
                    at = (slot, pl.ds(pl.multiple_of(r * 16, 16), 16), pl.ds(col, wide))
                    grad = gb[shape][at].astype(F32) * scale
                    mb[shape][at] = 0.9 * mb[shape][at] + 0.1 * grad
                    vb[shape][at] = 0.95 * vb[shape][at] + 0.05 * grad * grad

        before = [next((j for j in range(i - 1, -1, -1) if slots[j] == slots[i]), None) for i in range(len(todo))]
        ahead = min([i - j for i, j in enumerate(before) if j is not None], default=len(todo) + 2) - 2
        open_ = set(range(len(todo)))
        for i in range(-ahead, len(todo)):
            n = i + ahead
            if n < len(todo):
                if before[n] is not None:
                    wait(before[n], 1)
                    open_.discard(before[n])
                start(n, 0)
            if i >= 0:
                wait(i, 0)
                compute(i)
                start(i, 1)
        for i in sorted(open_):
            wait(i, 1)

    any_, dma = pl.BlockSpec(memory_space=pl.ANY), pltpu.SemaphoreType.DMA
    ms, vs, gs = ([x[n] for x in sets] for n in range(3))
    outs = [jax.ShapeDtypeStruct(x.shape, x.dtype) for x in (*copies, *ms, *vs)]
    scratch = [pltpu.VMEM((DEPTH, *x), BF16) for x in shapes]
    for dtype in (F32, F32, BF16):
        scratch += [pltpu.VMEM((MOMENT_DEPTH, *x), dtype) for x in kinds]
    if nc:
        scratch += [dma((len(shapes), DEPTH))] * 2
    scratch += [dma((len(kinds), 3, MOMENT_DEPTH)), dma((len(kinds), 2, MOMENT_DEPTH))]
    moved = sum(4 * x.size for x in copies) + sum(18 * x.size for x in ms)
    got = pl.pallas_call(
        run,
        name="finish",
        in_specs=[pl.BlockSpec(memory_space=pltpu.VMEM)] + [any_] * (nc + 3 * ns),
        out_specs=[any_] * len(outs),
        out_shape=outs,
        scratch_shapes=scratch,
        compiler_params=pltpu.CompilerParams(vmem_limit_bytes=ALL_VMEM),
        cost_estimate=pl.CostEstimate(flops=2 * moved, bytes_accessed=moved, transcendentals=0),
    )(factor, *copies, *ms, *vs, *gs)
    return got[:nc], got[nc : nc + ns], got[nc + ns :]


def fill(whole, far, mine, other):
    size = far.shape

    def copy(whole_ref, far_ref, mine_ref, other_ref, out_ref, buf, get, put):
        me = lax.axis_index("dp")
        z, core = me // 2, lax.rem(me, 2)
        is_end = (z == 0) | (z == 3)
        block = jnp.where(z < 2, 3, 0)

        def move(sources):
            first = [(2 * block + cc) * size[1] for cc in (core, 1 - core)]
            ins = [pltpu.make_async_copy(src, buf.at[i], get.at[i]) for i, src in enumerate(sources)]
            for one in ins:
                one.start()
            outs = []
            for i, one in enumerate(ins):
                one.wait()
                outs.append(pltpu.make_async_copy(buf.at[i], out_ref.at[:, pl.ds(pl.multiple_of(first[i], 16), size[1])], put.at[i]))
                outs[i].start()
            for one in outs:
                one.wait()

        @pl.when(is_end)
        def _():
            move((mine_ref, other_ref))

        @pl.when(jnp.logical_not(is_end))
        def _():
            move((far_ref,))

    any_ = pl.BlockSpec(memory_space=pl.ANY)
    return pl.pallas_call(
        copy,
        name="fill",
        in_specs=[any_] * 4,
        out_specs=any_,
        out_shape=jax.ShapeDtypeStruct(whole.shape, whole.dtype),
        scratch_shapes=[pltpu.VMEM((2, *size), whole.dtype)] + [pltpu.SemaphoreType.DMA((2,))] * 2,
        input_output_aliases={0: 0},
        compiler_params=pltpu.CompilerParams(vmem_limit_bytes=ALL_VMEM),
    )(whole, far, mine, other)


def solution(mesh):
    def step(*arrays):
        m, v = arrays[6:9], arrays[9:12]
        *rest, factor = exchange(*arrays)
        new, gradients, far = rest[:3], rest[3:6], rest[10]

        mine = lax.ppermute(far, "dp", [(2, 0), (3, 1), (4, 6), (5, 7)])
        sets = list(zip(m, v, gradients, strict=True))
        whole, new_m, new_v = finish(new, sets[:2], factor)
        mine, whole, new_m, new_v = lax.optimization_barrier((mine, whole, new_m, new_v))
        other = lax.ppermute(mine, "dp", [(0, 1), (1, 0), (6, 7), (7, 6)])
        _, last_m, last_v = finish([], sets[2:], factor)
        gate, up, down = whole
        up, other, last_m, last_v = lax.optimization_barrier((up, other, last_m, last_v))
        return (gate, fill(up, far, mine, other), down, *new_m, *last_m, *new_v, *last_v)

    all_of, cut = P(None, None, None), P(None, "dp", None)
    return jax.shard_map(
        step,
        mesh=mesh,
        in_specs=(P(("rep", "dp"), None, None, None),) * 3 + (all_of,) * 3 + (cut,) * 6,
        out_specs=(P("rep", None, None),) * 3 + (P("rep", "dp", None),) * 6,
        check_vma=False,
    )
```

```python
import functools

import jax
import jax.numpy as jnp
from jax import lax
from jax.experimental import pallas as pl
from jax.experimental.pallas import tpu as pltpu
from jax.sharding import PartitionSpec as P

MESH = pl.DeviceIdType.MESH
ALL_VMEM = 67043328
TILE = 16
RING = 8
SLOTS = 4
LAG = 2
PASS_LAG = 3
BEHIND = 16
SHAPES = ((128, 3200, 32, 640), (128, 3200, 32, 640), (400, 1024, 80, 1024))
SUBS = tuple(r // ch for r, _, ch, _ in SHAPES)
FIRST = (0, 4 * SUBS[0], 8 * SUBS[0], 8 * SUBS[0] + 4 * SUBS[2], 8 * SUBS[0] + 6 * SUBS[2])
STEPS = FIRST[4] + LAG
ORDER = (2, 0, 1)
OWN = {2: (0, 2 * SUBS[2]), 0: (2 * SUBS[2], 2 * (SUBS[2] + SUBS[0])), 1: (2 * (SUBS[2] + SUBS[0]), 2 * (SUBS[2] + 2 * SUBS[0]))}
BLOCK = OWN[1][1]
QUARTER = SHAPES[0][0] // 4
COUNT = 19660800.0
F32, BF16 = jnp.float32, jnp.bfloat16


def tiled(row):
    return pl.multiple_of(row, TILE)


def pieces(k, body):
    _, cols, ch, pc = SHAPES[k]

    @pl.loop(0, ch // TILE)
    def _(r):
        row = tiled(r * TILE)
        for col in range(0, cols, pc):
            body(row, col)


def kernel(*refs):
    g, w, m, v = (refs[3 * i : 3 * i + 3] for i in range(4))
    out, gown, moments, far, fac_out = refs[12:15], refs[15:18], refs[18:22], refs[22], refs[23]
    rest = list(refs[24:])

    def take(n):
        got, rest[:n] = tuple(rest[:n]), []
        return got

    inc, pb, wn = take(3), take(3), take(3)
    inc_near, own_a, own_b, wa, wb, ma, mb, va, vb, acc_a, acc_b, stat = take(12)
    recv1, part, wr, grecv = take(3), take(3), take(3), take(2)
    near_recv, own_sem, load_sem, psend, fsend, near_send, gsend, osend, isend, pwsend, pwrecv, local = take(12)
    stat_send, stat_recv, mv_send, mv_recv, mv_fan, mv_all, misc = take(7)

    rep, me = lax.axis_index("rep"), lax.axis_index("dp")
    z, c = me // 2, lax.rem(me, 2)
    dev = lambda zz, cc: (rep, 2 * zz + cc)
    partner = (rep, 2 * z + 1 - c)
    is_end = (z == 0) | (z == 3)
    is_mid = jnp.logical_not(is_end)
    left_half = z < 2
    zo = jnp.where(left_half, 0, 3)
    zm = jnp.where(left_half, 1, 2)
    zf = 3 - zm

    own = lambda k: own_a if k < 2 else own_b

    def remote(src, dst, send, recv, device):
        return pltpu.make_async_remote_copy(src_ref=src, dst_ref=dst, send_sem=send, recv_sem=recv, device_id=device, device_id_type=MESH)

    def rows(k, b, cc, s):
        r, _, ch, _ = SHAPES[k]
        return pl.ds(tiled((2 * b + cc) * r + s * ch), ch)

    def sub(k, s):
        ch = SHAPES[k][2]
        return pl.ds(tiled(s * ch), ch)

    barrier = pltpu.get_barrier_semaphore()
    for other in range(1, 8):
        pl.semaphore_signal(barrier, inc=1, device_id=(rep, lax.rem(me + other, 8)), device_id_type=MESH)
    for other in range(1, 4):
        pl.semaphore_signal(barrier, inc=1, device_id=(lax.rem(rep + other, 4), me), device_id_type=MESH)
    pl.semaphore_wait(barrier, 10)

    def quarter(ref, which, l):
        return ref.at[l, pl.ds(pl.multiple_of(which * QUARTER, QUARTER), QUARTER)]

    held = (m[0], m[1], v[0], v[1])

    @pl.when(is_mid)
    def _():
        for i in range(4):
            for l in range(2):
                remote(quarter(held[i], rep, l), quarter(moments[i], rep, l), mv_send.at[i], mv_recv.at[i, l], dev(zo, c)).start()

    def spread(j):
        for i in range(4):
            for l in range(2):
                @pl.when(j == 2 * i + l)
                def _():
                    here = quarter(moments[i], rep, l)
                    remote(here, here, mv_send.at[i], mv_recv.at[i, l], partner).wait_recv()
                    for other in range(1, 4):
                        remote(here, here, mv_fan.at[i], mv_all.at[i], (lax.rem(rep + other, 4), me)).start()

    def load(j, b, start):
        for k in ORDER:
            @pl.when((j >= OWN[k][0]) & (j < OWN[k][1]))
            def _():
                t = j - OWN[k][0]
                l, s, slot = t // SUBS[k], lax.rem(t, SUBS[k]), lax.rem(j, SLOTS)
                bufs = (wa, ma, va) if k < 2 else (wb, mb, vb)
                m_, v_ = (m[k], v[k]) if b is z else (moments[k], moments[2 + k]) if k < 2 else (None, None)
                if m_ is None:
                    return
                srcs = (w[k].at[l, rows(k, b, c, s)], m_.at[l, sub(k, s)], v_.at[l, sub(k, s)])
                for i in range(3):
                    copy = pltpu.make_async_copy(srcs[i], bufs[i].at[slot], load_sem.at[i, slot])
                    copy.start() if start else copy.wait()

    place = (z, 3 - z)
    after = (jnp.minimum(z + 1, 3), jnp.maximum(z - 1, 0))
    middle, end, near = (2, 1), (3, 0), (1, 2)

    def where_is(f, q, i):
        k = min(q, 2)
        t = i - FIRST[q]
        u, s = t // SUBS[k], lax.rem(t, SUBS[k])
        if q < 2:
            return k, jnp.where(u < 2, middle[f], end[f]), lax.rem(u, 2), s, True
        if q == 2:
            return k, jnp.where(u < 2, end[f], middle[f]), lax.rem(u, 2), s, (u < 2) | (place[f] < 2)
        return k, near[f], u, s, place[f] < 2

    def each_part(f, i, body):
        for q in range(4):
            k, b, l, s, active = where_is(f, q, i)

            @pl.when((i >= FIRST[q]) & (i < FIRST[q + 1]) & active)
            def _():
                body(q, k, b, l, s, lax.rem(i, RING))

    def fetch(f, i):
        def start(q, k, b, l, s, slot):
            remote(g[k].at[0, l, rows(k, b, 1 - c, s)], pb[k].at[b, l, sub(k, s)], psend.at[k], part[k].at[b, l, s], partner).start()
            pltpu.make_async_copy(g[k].at[0, l, rows(k, b, c, s)], own(k).at[f, slot], own_sem.at[f, slot]).start()

        each_part(f, i, start)

    def advance(f, i):
        def step(q, k, b, l, s, slot):
            here = (b, l, sub(k, s))
            pc = SHAPES[k][3]
            acc = acc_a if k < 2 else acc_b
            pltpu.make_async_copy(g[k].at[0, l, rows(k, b, c, s)], own(k).at[f, slot], own_sem.at[f, slot]).wait()
            remote(pb[k].at[here], pb[k].at[here], psend.at[k], part[k].at[b, l, s], partner).wait_recv()
            along = remote(pb[k].at[here], inc[k].at[here], fsend.at[f, k], recv1[k].at[b, l, s], dev(after[f], c))
            aside = remote(pb[k].at[here], inc_near.at[l, sub(k, s)], near_send, near_recv.at[l, s], dev(after[f], c))

            def total(into, arrived, squares=False):
                def body(row, col):
                    at = (pl.ds(row, TILE), pl.ds(col, pc))
                    down = pl.ds(tiled(s * SHAPES[k][2] + row), TILE)
                    to = (b, l, down, pl.ds(col, pc))
                    sum_ = own(k)[(f, slot, *at)].astype(F32) + pb[k][to].astype(F32)
                    if "line" in arrived:
                        sum_ = sum_ + inc[k][to].astype(F32)
                    if "near" in arrived:
                        sum_ = sum_ + inc_near[(l, down, pl.ds(col, pc))].astype(F32)
                    sum_ = sum_.astype(BF16)
                    into[k][to] = sum_
                    if squares:
                        rounded = sum_.astype(F32)
                        acc[...] += rounded * rounded

                pieces(k, body)

            if q == 3:

                @pl.when(place[f] == 0)
                def _():
                    total(pb, ())
                    aside.start()

                @pl.when(place[f] == 1)
                def _():
                    along.wait_recv()
                    aside.wait_recv()
                    total(inc, ("line", "near"), True)

                return

            @pl.when(place[f] == 0)
            def _():
                total(pb, ())

            @pl.when(place[f] > 0)
            def _():
                along.wait_recv()

            @pl.when((place[f] > 0) & (place[f] < 3))
            def _():
                total(pb, ("line",))

            @pl.when(place[f] < 3)
            def _():
                along.start()

            @pl.when(place[f] == 3)
            def _():
                total(inc, ("line",), True)

        each_part(f, i, step)

    def chunks(k, body):
        @pl.loop(0, 2 * SUBS[k])
        def _(t):
            body(t // SUBS[k], lax.rem(t, SUBS[k]))

    def back(k, l, s):
        here = inc[k].at[zm, l, sub(k, s)]
        remote(here, here, gsend.at[k], grecv[k].at[l, s], dev(zm, c)).start()

    acc_a[...] = jnp.zeros_like(acc_a)
    acc_b[...] = jnp.zeros_like(acc_b)

    @pl.loop(0, RING)
    def _(i):
        for f in range(2):
            fetch(f, i)

    @pl.loop(0, SLOTS)
    def _(j):
        load(j, z, True)

    @pl.loop(0, STEPS)
    def _(step):
        for f in range(2):
            i = step - LAG * place[f] - jnp.where(place[f] == 3, BEHIND, 0)

            @pl.when((i >= 0) & (i < FIRST[4]))
            def _():
                advance(f, i)
                fetch(f, i + RING)

        @pl.when(is_end & (step >= 4) & (lax.rem(step, 2) == 0))
        def _():
            spread(step // 2 - 2)

    def each_other(body):
        for other in range(1, 8):
            body(other - 1, lax.rem(me + other, 8))

    stat[me] = jnp.full((8, 128), jnp.sum(acc_a[...]) + jnp.sum(acc_b[...]), F32)
    each_other(lambda i, d: remote(stat.at[me], stat.at[me], stat_send.at[i], stat_recv.at[me], (rep, d)).start())

    @pl.when(is_end)
    def _():
        for k in range(2):
            chunks(k, functools.partial(back, k))

    each_other(lambda i, d: remote(stat.at[d], stat.at[d], stat_send.at[0], stat_recv.at[d], partner).wait_recv())
    squares = stat[0]
    for source in range(1, 8):
        squares = squares + stat[source]
    factor = jnp.minimum(1.0, 0.5 * lax.rsqrt(squares / COUNT + 1e-30))
    fac_out[...] = factor
    scale = factor[0:1, 0:1]

    def update(j, b, send, arrays=ORDER, last=BLOCK):
        load(j, b, False)
        for k in arrays:
            @pl.when((j >= OWN[k][0]) & (j < OWN[k][1]))
            def _():
                t = j - OWN[k][0]
                l, s, slot = t // SUBS[k], lax.rem(t, SUBS[k]), lax.rem(j, SLOTS)
                wx, mx, vx = (wa, ma, va) if k < 2 else (wb, mb, vb)
                _, _, ch, pc = SHAPES[k]
                which = 0 if b is z else 1

                if k < 2:

                    @pl.when(is_mid)
                    def _():
                        here = inc[k].at[z, l, sub(k, s)]
                        remote(here, here, gsend.at[k], grecv[k].at[l, s], partner).wait_recv()

                def body(row, col):
                    at = (slot, pl.ds(row, TILE), pl.ds(col, pc))
                    to = (l, pl.ds(tiled(s * ch + row), TILE), pl.ds(col, pc))
                    grad = inc[k][(b, *to)].astype(F32) * scale
                    new_m = 0.9 * mx[at] + 0.1 * grad
                    new_v = 0.95 * vx[at] + 0.05 * grad * grad
                    old = wx[at].astype(F32)
                    wn[k][(which, *to)] = (old - 0.02 * (new_m * lax.rsqrt(new_v + 1e-8) + 0.1 * old)).astype(BF16)

                pieces(k, body)
                src, dst = wn[k].at[which, l, sub(k, s)], out[k].at[l, rows(k, b, c, s)]
                send(k, l, s, src, dst)
                remote(src, dst, pwsend.at[k], pwrecv.at[k], partner).start()
                pltpu.make_async_copy(src, dst, local.at[k]).start()

        @pl.when(j + SLOTS < last)
        def _():
            load(j + SLOTS, b, True)

    def pass_index(j, b, to_sem, to, hop=None):
        for k in ORDER:
            @pl.when((j >= OWN[k][0]) & (j < OWN[k][1]))
            def _():
                t = j - OWN[k][0]
                l, s = t // SUBS[k], lax.rem(t, SUBS[k])
                there = out[k].at[l, rows(k, b, c, s)]
                aside = far.at[l, sub(k, s)] if k == 1 else None
                here = aside if k == 1 and hop == 3 else there
                remote(here, here, gsend.at[k], wr[k].at[b, l, s], partner).wait_recv()
                if to is not None and not (k == 1 and hop == 3):
                    remote(here, aside if k == 1 and hop == 2 else there, to_sem.at[k], wr[k].at[b, l, s], to).start()
                remote(here, there, pwsend.at[k], pwrecv.at[k], partner).start()

    def keep():
        for k in range(3):
            pltpu.make_async_copy(inc[k].at[z], gown[k], misc.at[k]).start()

    @pl.when(is_end)
    def _():
        inward = dev(zm, c)
        keep()

        @pl.loop(0, BLOCK)
        def _(j):
            update(j, z, lambda k, l, s, src, dst: remote(src, dst, isend.at[k], wr[k].at[z, l, s], inward).start())

        for i in range(4):
            three = moments[i].at[:, pl.ds(0, 3 * QUARTER)]
            remote(three, three, mv_fan.at[i], mv_all.at[i], partner).wait_recv()

        @pl.loop(OWN[0][0], OWN[0][0] + SLOTS)
        def _(j):
            load(j, zm, True)

        @pl.loop(OWN[0][0], BLOCK)
        def _(j):
            update(j, zm, lambda *_: None, (0, 1))

        @pl.loop(0, OWN[2][1])
        def _(j):
            pass_index(j, zm, None, None)
            pass_index(j, zf, None, None)

        @pl.loop(OWN[0][0], BLOCK)
        def _(j):
            pass_index(j, zf, None, None)

        @pl.loop(0, OWN[0][1])
        def _(j):
            pass_index(j, 3 - zo, None, None)

    @pl.when(is_mid)
    def _():
        outward, inward = dev(zo, c), dev(zf, c)

        def both(k, l, s, src, dst):
            if k == 2:
                remote(src, dst, osend.at[k], wr[k].at[z, l, s], outward).start()
            remote(src, dst, isend.at[k], wr[k].at[z, l, s], inward).start()

        @pl.loop(0, BLOCK + PASS_LAG)
        def _(j):
            @pl.when(j < BLOCK)
            def _():
                update(j, z, both)

            @pl.when(j >= PASS_LAG)
            def _():
                pass_index(j - PASS_LAG, zf, osend, outward)

        keep()

        @pl.loop(0, BLOCK + PASS_LAG)
        def _(j):
            @pl.when(j < BLOCK)
            def _():
                pass_index(j, zo, isend, inward, 2)

            @pl.when(j >= PASS_LAG)
            def _():
                pass_index(j - PASS_LAG, 3 - zo, osend, outward, 3)

    for k in range(3):
        r = SHAPES[k][0]
        blocks = lambda n: pb[k].at[pl.ds(0, n)]
        sent = lambda n, sem: remote(blocks(n), blocks(n), sem, pwrecv.at[k], partner).wait_send()
        sent(4, psend.at[k])
        for f in range(2):
            if k < 2:

                @pl.when(place[f] < 3)
                def _():
                    sent(2, fsend.at[f, k])

            else:

                @pl.when(place[f] < 2)
                def _():
                    sent(2, fsend.at[f, k])

                @pl.when(place[f] == 2)
                def _():
                    sent(1, fsend.at[f, k])

        def delivered(blocks_):
            half = out[k].at[:, pl.ds(0, blocks_ * r)]
            remote(half, half, gsend.at[k], pwrecv.at[k], partner).wait_recv()
            sent(blocks_, pwsend.at[k])

        def stored(n):
            pltpu.make_async_copy(pb[k].at[pl.ds(0, n)], pb[k].at[pl.ds(0, n)], local.at[k]).wait()

        @pl.when(is_end)
        def _():
            if k < 2:
                sent(1, gsend.at[k])
            sent(1, isend.at[k])
            delivered(3 if k == 1 else 4)
            stored(2 if k < 2 else 1)

        @pl.when(is_mid)
        def _():
            sent(1 if k == 1 else 3 if k == 2 else 2, osend.at[k])
            sent(2, isend.at[k])
            delivered(4)
            stored(1)

        pltpu.make_async_copy(inc[k].at[z], gown[k], misc.at[k]).wait()

    each_other(lambda i, d: remote(stat.at[me], stat.at[me], stat_send.at[i], stat_recv.at[me], (rep, d)).wait_send())

    @pl.when(is_end)
    def _():
        remote(inc_near, inc_near, near_send, mv_all.at[0], partner).wait_send()
        for i in range(4):
            three = moments[i].at[:, pl.ds(0, 3 * QUARTER)]
            remote(three, three, mv_fan.at[i], mv_all.at[i], partner).wait_send()

    @pl.when(is_mid)
    def _():
        for i in range(4):
            one = moments[i].at[:, pl.ds(0, QUARTER)]
            remote(one, one, mv_send.at[i], mv_all.at[i], partner).wait_send()


def exchange(*arrays):
    any_, dma = pl.BlockSpec(memory_space=pl.ANY), pltpu.SemaphoreType.DMA
    whole = [jax.ShapeDtypeStruct((2, 8 * r, n), BF16) for r, n, _, _ in SHAPES]
    block = [jax.ShapeDtypeStruct((2, r, n), BF16) for r, n, _, _ in SHAPES]
    moments = [jax.ShapeDtypeStruct((2, *SHAPES[0][:2]), F32)] * 4
    (_, na, ca, pa), (_, nb, cb, pc) = SHAPES[0], SHAPES[2]
    scratch = [pltpu.VMEM((4, 2, r, n), BF16) for r, n, _, _ in SHAPES] * 2
    scratch += [pltpu.VMEM((2 if r == SHAPES[0][0] else 1, 2, r, n), BF16) for r, n, _, _ in SHAPES]
    scratch += [pltpu.VMEM((2, *SHAPES[2][:2]), BF16)]
    scratch += [pltpu.VMEM((2, RING, ca, na), BF16), pltpu.VMEM((2, RING, cb, nb), BF16)]
    for dtype in (BF16, F32, F32):
        scratch += [pltpu.VMEM((SLOTS, ca, na), dtype), pltpu.VMEM((SLOTS, cb, nb), dtype)]
    scratch += [pltpu.VMEM((16, pa), F32), pltpu.VMEM((16, pc), F32), pltpu.VMEM((8, 8, 128), F32)]
    scratch += [dma((4, 2, s)) for s in SUBS] * 3 + [dma((2, s)) for s in SUBS[:2]]
    scratch += [dma((2, SUBS[2])), dma((2, RING)), dma((3, SLOTS)), dma((3,)), dma((2, 3)), dma, *[dma((3,))] * 6]
    scratch += [dma((7,)), dma((8,)), dma((4,)), dma((4, 2)), dma((4,)), dma((4,)), dma((3,))]
    return pl.pallas_call(
        kernel,
        name="exchange",
        out_shape=(*whole, *block, *moments, block[1], jax.ShapeDtypeStruct((8, 128), F32)),
        in_specs=[any_] * 12,
        out_specs=(*[any_] * 11, pl.BlockSpec(memory_space=pltpu.VMEM)),
        scratch_shapes=scratch,
        compiler_params=pltpu.CompilerParams(collective_id=0, has_side_effects=True, vmem_limit_bytes=ALL_VMEM),
    )(*arrays)


DEPTH = 6
MOMENT_DEPTH = 10


def finish(copies, sets, factor):
    nc, ns = len(copies), len(sets)
    size = [(x.shape[1] // 4, x.shape[2]) for x in copies]
    tall = [m.shape[1] // (4 if m.shape[1] % 64 == 0 else 5) for m, _, _ in sets]
    shapes = sorted(set(size), reverse=True)
    kinds = sorted({(t, m.shape[2]) for t, (m, _, _) in zip(tall, sets, strict=True)})
    todo = [("copy", k, l, p) for l in range(2) for p in range(4) for k in range(nc)]
    more = [("moment", k, l, p) for l in range(2) for k in range(ns) for p in range(sets[k][0].shape[1] // tall[k])]
    todo = [x for _, x in sorted([((i + 0.5) / len(todo), x) for i, x in enumerate(todo)] + [((i + 0.5) / len(more), x) for i, x in enumerate(more)])]

    def run(*refs):
        fac, refs = refs[0], list(refs[1:])

        def take(n):
            got, refs[:n] = tuple(refs[:n]), []
            return got

        src, ms, vs, gs, dst, new_m, new_v = (take(n) for n in (nc, ns, ns, ns, nc, ns, ns))
        bufs = take(len(shapes))
        mb, vb, gb = (take(len(kinds)) for _ in range(3))
        get, put = take(2) if nc else (None, None)
        mget, mput = take(2)
        scale = fac[0:1, 0:1]
        used, slots = {}, []
        for kind, k, _, _ in todo:
            shape = (kind, shapes.index(size[k]) if kind == "copy" else kinds.index((tall[k], sets[k][0].shape[2])))
            n = used.get(shape, 0)
            used[shape] = n + 1
            slots.append((*shape, n % (DEPTH if kind == "copy" else MOMENT_DEPTH)))

        def moves(i, way):
            (kind, k, l, p), (_, shape, slot) = todo[i], slots[i]
            if kind == "copy":
                at = (l, pl.ds(p * size[k][0], size[k][0]))
                buf = bufs[shape].at[slot]
                pairs = [(src[k].at[at], buf, get.at[shape, slot])] if way == 0 else [(buf, dst[k].at[at], put.at[shape, slot])]
            else:
                at = (l, pl.ds(p * tall[k], tall[k]))
                held = [x[shape].at[slot] for x in (mb, vb, gb)]
                if way == 0:
                    pairs = [(x[k].at[at], held[n], mget.at[shape, n, slot]) for n, x in enumerate((ms, vs, gs))]
                else:
                    pairs = [(held[n], x[k].at[at], mput.at[shape, n, slot]) for n, x in enumerate((new_m, new_v))]
            return [pltpu.make_async_copy(*pair) for pair in pairs]

        def start(i, way):
            for one in moves(i, way):
                one.start()

        def wait(i, way):
            for one in moves(i, way):
                one.wait()

        def compute(i):
            (kind, k, _, _), (_, shape, slot) = todo[i], slots[i]
            if kind == "copy":
                return
            wide = 640 if sets[k][0].shape[2] % 640 == 0 else 1024

            @pl.loop(0, tall[k] // TILE)
            def _(r):
                for col in range(0, sets[k][0].shape[2], wide):
                    at = (slot, pl.ds(tiled(r * TILE), TILE), pl.ds(col, wide))
                    grad = gb[shape][at].astype(F32) * scale
                    mb[shape][at] = 0.9 * mb[shape][at] + 0.1 * grad
                    vb[shape][at] = 0.95 * vb[shape][at] + 0.05 * grad * grad

        before = [next((j for j in range(i - 1, -1, -1) if slots[j] == slots[i]), None) for i in range(len(todo))]
        ahead = min([i - j for i, j in enumerate(before) if j is not None], default=len(todo) + 2) - 2
        open_ = set(range(len(todo)))
        for i in range(-ahead, len(todo)):
            n = i + ahead
            if n < len(todo):
                if before[n] is not None:
                    wait(before[n], 1)
                    open_.discard(before[n])
                start(n, 0)
            if i >= 0:
                wait(i, 0)
                compute(i)
                start(i, 1)
        for i in sorted(open_):
            wait(i, 1)

    any_, dma = pl.BlockSpec(memory_space=pl.ANY), pltpu.SemaphoreType.DMA
    ms, vs, gs = ([x[n] for x in sets] for n in range(3))
    outs = [jax.ShapeDtypeStruct(x.shape, x.dtype) for x in (*copies, *ms, *vs)]
    scratch = [pltpu.VMEM((DEPTH, *x), BF16) for x in shapes]
    for dtype in (F32, F32, BF16):
        scratch += [pltpu.VMEM((MOMENT_DEPTH, *x), dtype) for x in kinds]
    if nc:
        scratch += [dma((len(shapes), DEPTH))] * 2
    scratch += [dma((len(kinds), 3, MOMENT_DEPTH)), dma((len(kinds), 2, MOMENT_DEPTH))]
    moved = sum(4 * x.size for x in copies) + sum(18 * x.size for x in ms)
    got = pl.pallas_call(
        run,
        name="finish",
        in_specs=[pl.BlockSpec(memory_space=pltpu.VMEM)] + [any_] * (nc + 3 * ns),
        out_specs=[any_] * len(outs),
        out_shape=outs,
        scratch_shapes=scratch,
        compiler_params=pltpu.CompilerParams(vmem_limit_bytes=ALL_VMEM),
        cost_estimate=pl.CostEstimate(flops=2 * moved, bytes_accessed=moved, transcendentals=0),
    )(factor, *copies, *ms, *vs, *gs)
    return got[:nc], got[nc : nc + ns], got[nc + ns :]


def fill(whole, far, mine, other):
    size = far.shape

    def copy(whole_ref, far_ref, mine_ref, other_ref, out_ref, buf, get, put):
        me = lax.axis_index("dp")
        z, core = me // 2, lax.rem(me, 2)
        is_end = (z == 0) | (z == 3)
        block = jnp.where(z < 2, 3, 0)

        def move(sources):
            first = [(2 * block + cc) * size[1] for cc in (core, 1 - core)]
            ins = [pltpu.make_async_copy(src, buf.at[i], get.at[i]) for i, src in enumerate(sources)]
            for one in ins:
                one.start()
            outs = []
            for i, one in enumerate(ins):
                one.wait()
                outs.append(pltpu.make_async_copy(buf.at[i], out_ref.at[:, pl.ds(tiled(first[i]), size[1])], put.at[i]))
                outs[i].start()
            for one in outs:
                one.wait()

        @pl.when(is_end)
        def _():
            move((mine_ref, other_ref))

        @pl.when(jnp.logical_not(is_end))
        def _():
            move((far_ref,))

    any_ = pl.BlockSpec(memory_space=pl.ANY)
    return pl.pallas_call(
        copy,
        name="fill",
        in_specs=[any_] * 4,
        out_specs=any_,
        out_shape=jax.ShapeDtypeStruct(whole.shape, whole.dtype),
        scratch_shapes=[pltpu.VMEM((2, *size), whole.dtype)] + [pltpu.SemaphoreType.DMA((2,))] * 2,
        input_output_aliases={0: 0},
        compiler_params=pltpu.CompilerParams(vmem_limit_bytes=ALL_VMEM),
    )(whole, far, mine, other)


def solution(mesh):
    def step(*arrays):
        m, v = arrays[6:9], arrays[9:12]
        *rest, factor = exchange(*arrays)
        new, gradients, far = rest[:3], rest[3:6], rest[10]

        mine = lax.ppermute(far, "dp", [(2, 0), (3, 1), (4, 6), (5, 7)])
        sets = list(zip(m, v, gradients, strict=True))
        whole, new_m, new_v = finish(new, sets[:2], factor)
        mine, whole, new_m, new_v = lax.optimization_barrier((mine, whole, new_m, new_v))
        other = lax.ppermute(mine, "dp", [(0, 1), (1, 0), (6, 7), (7, 6)])
        _, last_m, last_v = finish([], sets[2:], factor)
        gate, up, down = whole
        up, other, last_m, last_v = lax.optimization_barrier((up, other, last_m, last_v))
        return (gate, fill(up, far, mine, other), down, *new_m, *last_m, *new_v, *last_v)

    all_of, cut = P(), P(None, "dp")
    return jax.shard_map(
        step,
        mesh=mesh,
        in_specs=(P(("rep", "dp")),) * 3 + (all_of,) * 3 + (cut,) * 6,
        out_specs=(P("rep"),) * 3 + (P("rep", "dp"),) * 6,
        check_vma=False,
    )
```

```python
import functools

import jax
import jax.numpy as jnp
from jax import lax
from jax.experimental import pallas as pl
from jax.experimental.pallas import tpu as pltpu
from jax.sharding import PartitionSpec as P

MESH = pl.DeviceIdType.MESH
ALL_VMEM = 67043328
TILE = 16
RING = 8
SLOTS = 4
LAG = 2
PASS_LAG = 3
BEHIND = 16
SHAPES = ((128, 3200, 32, 640), (128, 3200, 32, 640), (400, 1024, 80, 1024))
SUBS = tuple(r // ch for r, _, ch, _ in SHAPES)
FIRST = (0, 4 * SUBS[0], 8 * SUBS[0], 8 * SUBS[0] + 4 * SUBS[2], 8 * SUBS[0] + 6 * SUBS[2])
STEPS = FIRST[4] + LAG
ORDER = (2, 0, 1)
OWN = {2: (0, 2 * SUBS[2]), 0: (2 * SUBS[2], 2 * (SUBS[2] + SUBS[0])), 1: (2 * (SUBS[2] + SUBS[0]), 2 * (SUBS[2] + 2 * SUBS[0]))}
BLOCK = OWN[1][1]
QUARTER = SHAPES[0][0] // 4
COUNT = 19660800.0
F32, BF16 = jnp.float32, jnp.bfloat16


def tiled(row):
    return pl.multiple_of(row, TILE)


def pieces(k, body):
    _, cols, ch, pc = SHAPES[k]

    @pl.loop(0, ch // TILE)
    def _(r):
        row = tiled(r * TILE)
        for col in range(0, cols, pc):
            body(row, col)


def kernel(*refs):
    g, w, m, v = (refs[3 * i : 3 * i + 3] for i in range(4))
    out, gown, moments, far, fac_out = refs[12:15], refs[15:18], refs[18:22], refs[22], refs[23]
    rest = list(refs[24:])

    def take(n):
        got, rest[:n] = tuple(rest[:n]), []
        return got

    inc, pb, wn = take(3), take(3), take(3)
    inc_near, own_a, own_b, wa, wb, ma, mb, va, vb, acc_a, acc_b, stat = take(12)
    recv1, part, wr, grecv = take(3), take(3), take(3), take(2)
    near_recv, own_sem, load_sem, psend, fsend, near_send, gsend, osend, isend, pwsend, pwrecv, local = take(12)
    stat_send, stat_recv, mv_send, mv_recv, mv_fan, mv_all, misc = take(7)

    rep, me = lax.axis_index("rep"), lax.axis_index("dp")
    z, c = me // 2, lax.rem(me, 2)
    dev = lambda zz, cc: (rep, 2 * zz + cc)
    partner = (rep, 2 * z + 1 - c)
    is_end = (z == 0) | (z == 3)
    is_mid = jnp.logical_not(is_end)
    left_half = z < 2
    zo = jnp.where(left_half, 0, 3)
    zm = jnp.where(left_half, 1, 2)
    zf = 3 - zm

    own = lambda k: own_a if k < 2 else own_b

    def remote(src, dst, send, recv, device):
        return pltpu.make_async_remote_copy(src_ref=src, dst_ref=dst, send_sem=send, recv_sem=recv, device_id=device, device_id_type=MESH)

    def rows(k, b, cc, s):
        r, _, ch, _ = SHAPES[k]
        return pl.ds(tiled((2 * b + cc) * r + s * ch), ch)

    def sub(k, s):
        ch = SHAPES[k][2]
        return pl.ds(tiled(s * ch), ch)

    barrier = pltpu.get_barrier_semaphore()
    for other in range(1, 8):
        pl.semaphore_signal(barrier, inc=1, device_id=(rep, lax.rem(me + other, 8)), device_id_type=MESH)
    for other in range(1, 4):
        pl.semaphore_signal(barrier, inc=1, device_id=(lax.rem(rep + other, 4), me), device_id_type=MESH)
    pl.semaphore_wait(barrier, 10)

    def quarter(ref, which, l):
        return ref.at[l, pl.ds(pl.multiple_of(which * QUARTER, QUARTER), QUARTER)]

    held = (m[0], m[1], v[0], v[1])

    @pl.when(is_mid)
    def _():
        for i in range(4):
            for l in range(2):
                remote(quarter(held[i], rep, l), quarter(moments[i], rep, l), mv_send.at[i], mv_recv.at[i, l], dev(zo, c)).start()

    def spread(j):
        for i in range(4):
            for l in range(2):
                @pl.when(j == 2 * i + l)
                def _():
                    here = quarter(moments[i], rep, l)
                    remote(here, here, mv_send.at[i], mv_recv.at[i, l], partner).wait_recv()
                    for other in range(1, 4):
                        remote(here, here, mv_fan.at[i], mv_all.at[i], (lax.rem(rep + other, 4), me)).start()

    def load(j, b, start):
        for k in ORDER:
            @pl.when((j >= OWN[k][0]) & (j < OWN[k][1]))
            def _():
                t = j - OWN[k][0]
                l, s, slot = t // SUBS[k], lax.rem(t, SUBS[k]), lax.rem(j, SLOTS)
                bufs = (wa, ma, va) if k < 2 else (wb, mb, vb)
                m_, v_ = (m[k], v[k]) if b is z else (moments[k], moments[2 + k]) if k < 2 else (None, None)
                if m_ is None:
                    return
                srcs = (w[k].at[l, rows(k, b, c, s)], m_.at[l, sub(k, s)], v_.at[l, sub(k, s)])
                for i in range(3):
                    copy = pltpu.make_async_copy(srcs[i], bufs[i].at[slot], load_sem.at[i, slot])
                    copy.start() if start else copy.wait()

    place = (z, 3 - z)
    after = (jnp.minimum(z + 1, 3), jnp.maximum(z - 1, 0))
    middle, end, near = (2, 1), (3, 0), (1, 2)

    def where_is(f, q, i):
        k = min(q, 2)
        t = i - FIRST[q]
        u, s = t // SUBS[k], lax.rem(t, SUBS[k])
        if q < 2:
            return k, jnp.where(u < 2, middle[f], end[f]), lax.rem(u, 2), s, True
        if q == 2:
            return k, jnp.where(u < 2, end[f], middle[f]), lax.rem(u, 2), s, (u < 2) | (place[f] < 2)
        return k, near[f], u, s, place[f] < 2

    def each_part(f, i, body):
        for q in range(4):
            k, b, l, s, active = where_is(f, q, i)

            @pl.when((i >= FIRST[q]) & (i < FIRST[q + 1]) & active)
            def _():
                body(q, k, b, l, s, lax.rem(i, RING))

    def fetch(f, i):
        def start(q, k, b, l, s, slot):
            remote(g[k].at[0, l, rows(k, b, 1 - c, s)], pb[k].at[b, l, sub(k, s)], psend.at[k], part[k].at[b, l, s], partner).start()
            pltpu.make_async_copy(g[k].at[0, l, rows(k, b, c, s)], own(k).at[f, slot], own_sem.at[f, slot]).start()

        each_part(f, i, start)

    def advance(f, i):
        def step(q, k, b, l, s, slot):
            here = (b, l, sub(k, s))
            pc = SHAPES[k][3]
            acc = acc_a if k < 2 else acc_b
            pltpu.make_async_copy(g[k].at[0, l, rows(k, b, c, s)], own(k).at[f, slot], own_sem.at[f, slot]).wait()
            remote(pb[k].at[here], pb[k].at[here], psend.at[k], part[k].at[b, l, s], partner).wait_recv()
            along = remote(pb[k].at[here], inc[k].at[here], fsend.at[f, k], recv1[k].at[b, l, s], dev(after[f], c))
            aside = remote(pb[k].at[here], inc_near.at[l, sub(k, s)], near_send, near_recv.at[l, s], dev(after[f], c))

            def total(into, arrived, squares=False):
                def body(row, col):
                    at = (pl.ds(row, TILE), pl.ds(col, pc))
                    down = pl.ds(tiled(s * SHAPES[k][2] + row), TILE)
                    to = (b, l, down, pl.ds(col, pc))
                    sum_ = own(k)[(f, slot, *at)].astype(F32) + pb[k][to].astype(F32)
                    if "line" in arrived:
                        sum_ = sum_ + inc[k][to].astype(F32)
                    if "near" in arrived:
                        sum_ = sum_ + inc_near[(l, down, pl.ds(col, pc))].astype(F32)
                    sum_ = sum_.astype(BF16)
                    into[k][to] = sum_
                    if squares:
                        rounded = sum_.astype(F32)
                        acc[...] += rounded * rounded

                pieces(k, body)

            if q == 3:

                @pl.when(place[f] == 0)
                def _():
                    total(pb, ())
                    aside.start()

                @pl.when(place[f] == 1)
                def _():
                    along.wait_recv()
                    aside.wait_recv()
                    total(inc, ("line", "near"), True)

                return

            @pl.when(place[f] == 0)
            def _():
                total(pb, ())

            @pl.when(place[f] > 0)
            def _():
                along.wait_recv()

            @pl.when((place[f] > 0) & (place[f] < 3))
            def _():
                total(pb, ("line",))

            @pl.when(place[f] < 3)
            def _():
                along.start()

            @pl.when(place[f] == 3)
            def _():
                total(inc, ("line",), True)

        each_part(f, i, step)

    def chunks(k, body):
        @pl.loop(0, 2 * SUBS[k])
        def _(t):
            body(t // SUBS[k], lax.rem(t, SUBS[k]))

    def back(k, l, s):
        here = inc[k].at[zm, l, sub(k, s)]
        remote(here, here, gsend.at[k], grecv[k].at[l, s], dev(zm, c)).start()

    acc_a[...] = jnp.zeros_like(acc_a)
    acc_b[...] = jnp.zeros_like(acc_b)

    @pl.loop(0, RING)
    def _(i):
        for f in range(2):
            fetch(f, i)

    @pl.loop(0, SLOTS)
    def _(j):
        load(j, z, True)

    @pl.loop(0, STEPS)
    def _(step):
        for f in range(2):
            i = step - LAG * place[f] - jnp.where(place[f] == 3, BEHIND, 0)

            @pl.when((i >= 0) & (i < FIRST[4]))
            def _():
                advance(f, i)
                fetch(f, i + RING)

        @pl.when(is_end & (step >= 4) & (lax.rem(step, 2) == 0))
        def _():
            spread(step // 2 - 2)

    def each_other(body):
        for other in range(1, 8):
            body(other - 1, lax.rem(me + other, 8))

    stat[me] = jnp.full((8, 128), jnp.sum(acc_a[...]) + jnp.sum(acc_b[...]), F32)
    each_other(lambda i, d: remote(stat.at[me], stat.at[me], stat_send.at[i], stat_recv.at[me], (rep, d)).start())

    @pl.when(is_end)
    def _():
        for k in range(2):
            chunks(k, functools.partial(back, k))

    each_other(lambda i, d: remote(stat.at[d], stat.at[d], stat_send.at[0], stat_recv.at[d], partner).wait_recv())
    squares = stat[0]
    for source in range(1, 8):
        squares = squares + stat[source]
    factor = jnp.minimum(1.0, 0.5 * lax.rsqrt(squares / COUNT + 1e-30))
    fac_out[...] = factor
    scale = factor[0:1, 0:1]

    def update(j, b, send, arrays=ORDER, last=BLOCK):
        load(j, b, False)
        for k in arrays:
            @pl.when((j >= OWN[k][0]) & (j < OWN[k][1]))
            def _():
                t = j - OWN[k][0]
                l, s, slot = t // SUBS[k], lax.rem(t, SUBS[k]), lax.rem(j, SLOTS)
                wx, mx, vx = (wa, ma, va) if k < 2 else (wb, mb, vb)
                _, _, ch, pc = SHAPES[k]
                which = 0 if b is z else 1

                if k < 2:

                    @pl.when(is_mid)
                    def _():
                        here = inc[k].at[z, l, sub(k, s)]
                        remote(here, here, gsend.at[k], grecv[k].at[l, s], partner).wait_recv()

                def body(row, col):
                    at = (slot, pl.ds(row, TILE), pl.ds(col, pc))
                    to = (l, pl.ds(tiled(s * ch + row), TILE), pl.ds(col, pc))
                    grad = inc[k][(b, *to)].astype(F32) * scale
                    new_m = 0.9 * mx[at] + 0.1 * grad
                    new_v = 0.95 * vx[at] + 0.05 * grad * grad
                    old = wx[at].astype(F32)
                    wn[k][(which, *to)] = (old - 0.02 * (new_m * lax.rsqrt(new_v + 1e-8) + 0.1 * old)).astype(BF16)

                pieces(k, body)
                src, dst = wn[k].at[which, l, sub(k, s)], out[k].at[l, rows(k, b, c, s)]
                send(k, l, s, src, dst)
                remote(src, dst, pwsend.at[k], pwrecv.at[k], partner).start()
                pltpu.make_async_copy(src, dst, local.at[k]).start()

        @pl.when(j + SLOTS < last)
        def _():
            load(j + SLOTS, b, True)

    def pass_index(j, b, to_sem, to, hop=None):
        for k in ORDER:
            @pl.when((j >= OWN[k][0]) & (j < OWN[k][1]))
            def _():
                t = j - OWN[k][0]
                l, s = t // SUBS[k], lax.rem(t, SUBS[k])
                there = out[k].at[l, rows(k, b, c, s)]
                aside = far.at[l, sub(k, s)] if k == 1 else None
                here = aside if k == 1 and hop == 3 else there
                remote(here, here, gsend.at[k], wr[k].at[b, l, s], partner).wait_recv()
                if to is not None and not (k == 1 and hop == 3):
                    remote(here, aside if k == 1 and hop == 2 else there, to_sem.at[k], wr[k].at[b, l, s], to).start()
                remote(here, there, pwsend.at[k], pwrecv.at[k], partner).start()

    def keep():
        for k in range(3):
            pltpu.make_async_copy(inc[k].at[z], gown[k], misc.at[k]).start()

    @pl.when(is_end)
    def _():
        inward = dev(zm, c)
        keep()

        @pl.loop(0, BLOCK)
        def _(j):
            update(j, z, lambda k, l, s, src, dst: remote(src, dst, isend.at[k], wr[k].at[z, l, s], inward).start())

        for i in range(4):
            three = moments[i].at[:, pl.ds(0, 3 * QUARTER)]
            remote(three, three, mv_fan.at[i], mv_all.at[i], partner).wait_recv()

        @pl.loop(OWN[0][0], OWN[0][0] + SLOTS)
        def _(j):
            load(j, zm, True)

        @pl.loop(OWN[0][0], BLOCK)
        def _(j):
            update(j, zm, lambda *_: None, (0, 1))

        @pl.loop(0, OWN[2][1])
        def _(j):
            pass_index(j, zm, None, None)
            pass_index(j, zf, None, None)

        @pl.loop(OWN[0][0], BLOCK)
        def _(j):
            pass_index(j, zf, None, None)

        @pl.loop(0, OWN[0][1])
        def _(j):
            pass_index(j, 3 - zo, None, None)

    @pl.when(is_mid)
    def _():
        outward, inward = dev(zo, c), dev(zf, c)

        def both(k, l, s, src, dst):
            if k == 2:
                remote(src, dst, osend.at[k], wr[k].at[z, l, s], outward).start()
            remote(src, dst, isend.at[k], wr[k].at[z, l, s], inward).start()

        @pl.loop(0, BLOCK + PASS_LAG)
        def _(j):
            @pl.when(j < BLOCK)
            def _():
                update(j, z, both)

            @pl.when(j >= PASS_LAG)
            def _():
                pass_index(j - PASS_LAG, zf, osend, outward)

        keep()

        @pl.loop(0, BLOCK + PASS_LAG)
        def _(j):
            @pl.when(j < BLOCK)
            def _():
                pass_index(j, zo, isend, inward, 2)

            @pl.when(j >= PASS_LAG)
            def _():
                pass_index(j - PASS_LAG, 3 - zo, osend, outward, 3)

    for k in range(3):
        r = SHAPES[k][0]
        blocks = lambda n: pb[k].at[pl.ds(0, n)]
        sent = lambda n, sem: remote(blocks(n), blocks(n), sem, pwrecv.at[k], partner).wait_send()
        sent(4, psend.at[k])
        for f in range(2):
            if k < 2:

                @pl.when(place[f] < 3)
                def _():
                    sent(2, fsend.at[f, k])

            else:

                @pl.when(place[f] < 2)
                def _():
                    sent(2, fsend.at[f, k])

                @pl.when(place[f] == 2)
                def _():
                    sent(1, fsend.at[f, k])

        def delivered(blocks_):
            half = out[k].at[:, pl.ds(0, blocks_ * r)]
            remote(half, half, gsend.at[k], pwrecv.at[k], partner).wait_recv()
            sent(blocks_, pwsend.at[k])

        def stored(n):
            pltpu.make_async_copy(pb[k].at[pl.ds(0, n)], pb[k].at[pl.ds(0, n)], local.at[k]).wait()

        @pl.when(is_end)
        def _():
            if k < 2:
                sent(1, gsend.at[k])
            sent(1, isend.at[k])
            delivered(3 if k == 1 else 4)
            stored(2 if k < 2 else 1)

        @pl.when(is_mid)
        def _():
            sent(1 if k == 1 else 3 if k == 2 else 2, osend.at[k])
            sent(2, isend.at[k])
            delivered(4)
            stored(1)

        pltpu.make_async_copy(inc[k].at[z], gown[k], misc.at[k]).wait()

    each_other(lambda i, d: remote(stat.at[me], stat.at[me], stat_send.at[i], stat_recv.at[me], (rep, d)).wait_send())

    @pl.when(is_end)
    def _():
        remote(inc_near, inc_near, near_send, mv_all.at[0], partner).wait_send()
        for i in range(4):
            three = moments[i].at[:, pl.ds(0, 3 * QUARTER)]
            remote(three, three, mv_fan.at[i], mv_all.at[i], partner).wait_send()

    @pl.when(is_mid)
    def _():
        for i in range(4):
            one = moments[i].at[:, pl.ds(0, QUARTER)]
            remote(one, one, mv_send.at[i], mv_all.at[i], partner).wait_send()


def exchange(*arrays):
    any_, dma = pl.BlockSpec(memory_space=pl.ANY), pltpu.SemaphoreType.DMA
    whole = [jax.ShapeDtypeStruct((2, 8 * r, n), BF16) for r, n, _, _ in SHAPES]
    block = [jax.ShapeDtypeStruct((2, r, n), BF16) for r, n, _, _ in SHAPES]
    moments = [jax.ShapeDtypeStruct((2, *SHAPES[0][:2]), F32)] * 4
    (_, na, ca, pa), (_, nb, cb, pc) = SHAPES[0], SHAPES[2]
    scratch = [pltpu.VMEM((4, 2, r, n), BF16) for r, n, _, _ in SHAPES] * 2
    scratch += [pltpu.VMEM((2 if r == SHAPES[0][0] else 1, 2, r, n), BF16) for r, n, _, _ in SHAPES]
    scratch += [pltpu.VMEM((2, *SHAPES[2][:2]), BF16)]
    scratch += [pltpu.VMEM((2, RING, ca, na), BF16), pltpu.VMEM((2, RING, cb, nb), BF16)]
    for dtype in (BF16, F32, F32):
        scratch += [pltpu.VMEM((SLOTS, ca, na), dtype), pltpu.VMEM((SLOTS, cb, nb), dtype)]
    scratch += [pltpu.VMEM((16, pa), F32), pltpu.VMEM((16, pc), F32), pltpu.VMEM((8, 8, 128), F32)]
    scratch += [dma((4, 2, s)) for s in SUBS] * 3 + [dma((2, s)) for s in SUBS[:2]]
    scratch += [dma((2, SUBS[2])), dma((2, RING)), dma((3, SLOTS)), dma((3,)), dma((2, 3)), dma, *[dma((3,))] * 6]
    scratch += [dma((7,)), dma((8,)), dma((4,)), dma((4, 2)), dma((4,)), dma((4,)), dma((3,))]
    return pl.pallas_call(
        kernel,
        name="exchange",
        out_shape=(*whole, *block, *moments, block[1], jax.ShapeDtypeStruct((8, 128), F32)),
        in_specs=[any_] * 12,
        out_specs=(*[any_] * 11, pl.BlockSpec(memory_space=pltpu.VMEM)),
        scratch_shapes=scratch,
        compiler_params=pltpu.CompilerParams(collective_id=0, has_side_effects=True, vmem_limit_bytes=ALL_VMEM),
    )(*arrays)


DEPTH = 6
MOMENT_DEPTH = 10


def finish(copies, sets, factor):
    nc, ns = len(copies), len(sets)
    size = [(x.shape[1] // 4, x.shape[2]) for x in copies]
    tall = [m.shape[1] // (4 if m.shape[1] % 64 == 0 else 5) for m, _, _ in sets]
    shapes = sorted(set(size), reverse=True)
    kinds = sorted({(t, m.shape[2]) for t, (m, _, _) in zip(tall, sets, strict=True)})
    todo = [("copy", k, l, p) for l in range(2) for p in range(4) for k in range(nc)]
    more = [("moment", k, l, p) for l in range(2) for k in range(ns) for p in range(sets[k][0].shape[1] // tall[k])]
    todo = [x for _, x in sorted([((i + 0.5) / len(todo), x) for i, x in enumerate(todo)] + [((i + 0.5) / len(more), x) for i, x in enumerate(more)])]

    def run(*refs):
        fac, refs = refs[0], list(refs[1:])

        def take(n):
            got, refs[:n] = tuple(refs[:n]), []
            return got

        src, ms, vs, gs, dst, new_m, new_v = (take(n) for n in (nc, ns, ns, ns, nc, ns, ns))
        bufs = take(len(shapes))
        mb, vb, gb = (take(len(kinds)) for _ in range(3))
        get, put = take(2) if nc else (None, None)
        mget, mput = take(2)
        scale = fac[0:1, 0:1]
        used, slots = {}, []
        for kind, k, _, _ in todo:
            shape = (kind, shapes.index(size[k]) if kind == "copy" else kinds.index((tall[k], sets[k][0].shape[2])))
            n = used.get(shape, 0)
            used[shape] = n + 1
            slots.append((*shape, n % (DEPTH if kind == "copy" else MOMENT_DEPTH)))

        def moves(i, way):
            (kind, k, l, p), (_, shape, slot) = todo[i], slots[i]
            if kind == "copy":
                at = (l, pl.ds(p * size[k][0], size[k][0]))
                buf = bufs[shape].at[slot]
                pairs = [(src[k].at[at], buf, get.at[shape, slot])] if way == 0 else [(buf, dst[k].at[at], put.at[shape, slot])]
            else:
                at = (l, pl.ds(p * tall[k], tall[k]))
                held = [x[shape].at[slot] for x in (mb, vb, gb)]
                if way == 0:
                    pairs = [(x[k].at[at], held[n], mget.at[shape, n, slot]) for n, x in enumerate((ms, vs, gs))]
                else:
                    pairs = [(held[n], x[k].at[at], mput.at[shape, n, slot]) for n, x in enumerate((new_m, new_v))]
            return [pltpu.make_async_copy(*pair) for pair in pairs]

        def start(i, way):
            for one in moves(i, way):
                one.start()

        def wait(i, way):
            for one in moves(i, way):
                one.wait()

        def compute(i):
            (kind, k, _, _), (_, shape, slot) = todo[i], slots[i]
            if kind == "copy":
                return
            wide = 640 if sets[k][0].shape[2] % 640 == 0 else 1024

            @pl.loop(0, tall[k] // TILE)
            def _(r):
                for col in range(0, sets[k][0].shape[2], wide):
                    at = (slot, pl.ds(tiled(r * TILE), TILE), pl.ds(col, wide))
                    grad = gb[shape][at].astype(F32) * scale
                    mb[shape][at] = 0.9 * mb[shape][at] + 0.1 * grad
                    vb[shape][at] = 0.95 * vb[shape][at] + 0.05 * grad * grad

        before = [next((j for j in range(i - 1, -1, -1) if slots[j] == slots[i]), None) for i in range(len(todo))]
        ahead = min([i - j for i, j in enumerate(before) if j is not None], default=len(todo) + 2) - 2
        open_ = set(range(len(todo)))
        for i in range(-ahead, len(todo)):
            n = i + ahead
            if n < len(todo):
                if before[n] is not None:
                    wait(before[n], 1)
                    open_.discard(before[n])
                start(n, 0)
            if i >= 0:
                wait(i, 0)
                compute(i)
                start(i, 1)
        for i in sorted(open_):
            wait(i, 1)

    any_, dma = pl.BlockSpec(memory_space=pl.ANY), pltpu.SemaphoreType.DMA
    ms, vs, gs = ([x[n] for x in sets] for n in range(3))
    outs = [jax.ShapeDtypeStruct(x.shape, x.dtype) for x in (*copies, *ms, *vs)]
    scratch = [pltpu.VMEM((DEPTH, *x), BF16) for x in shapes]
    for dtype in (F32, F32, BF16):
        scratch += [pltpu.VMEM((MOMENT_DEPTH, *x), dtype) for x in kinds]
    if nc:
        scratch += [dma((len(shapes), DEPTH))] * 2
    scratch += [dma((len(kinds), 3, MOMENT_DEPTH)), dma((len(kinds), 2, MOMENT_DEPTH))]
    moved = sum(4 * x.size for x in copies) + sum(18 * x.size for x in ms)
    got = pl.pallas_call(
        run,
        name="finish",
        in_specs=[pl.BlockSpec(memory_space=pltpu.VMEM)] + [any_] * (nc + 3 * ns),
        out_specs=[any_] * len(outs),
        out_shape=outs,
        scratch_shapes=scratch,
        compiler_params=pltpu.CompilerParams(vmem_limit_bytes=ALL_VMEM),
        cost_estimate=pl.CostEstimate(flops=2 * moved, bytes_accessed=moved, transcendentals=0),
    )(factor, *copies, *ms, *vs, *gs)
    return got[:nc], got[nc : nc + ns], got[nc + ns :]


def fill(whole, middle, end, other):
    size = end.shape

    def copy(whole_ref, middle_ref, end_ref, out_ref, buf, get, put):
        me = lax.axis_index("dp")
        z, core = me // 2, lax.rem(me, 2)
        is_end = (z == 0) | (z == 3)
        block = jnp.where(z < 2, 3, 0)
        first = (2 * block + (1 - core if other else core)) * size[1]

        def move(src):
            ins = [pltpu.make_async_copy(src.at[l], buf.at[l], get.at[l]) for l in range(2)]
            outs = [pltpu.make_async_copy(buf.at[l], out_ref.at[l, pl.ds(tiled(first), size[1])], put.at[l]) for l in range(2)]
            for one in ins:
                one.start()
            for l in range(2):
                ins[l].wait()
                outs[l].start()
            for one in outs:
                one.wait()

        @pl.when(is_end)
        def _():
            move(end_ref)

        if not other:

            @pl.when(jnp.logical_not(is_end))
            def _():
                move(middle_ref)

    any_ = pl.BlockSpec(memory_space=pl.ANY)
    return pl.pallas_call(
        copy,
        name="fill",
        in_specs=[any_] * 3,
        out_specs=any_,
        out_shape=jax.ShapeDtypeStruct(whole.shape, whole.dtype),
        scratch_shapes=[pltpu.VMEM(size, whole.dtype)] + [pltpu.SemaphoreType.DMA((2,))] * 2,
        input_output_aliases={0: 0},
        compiler_params=pltpu.CompilerParams(vmem_limit_bytes=ALL_VMEM),
        cost_estimate=pl.CostEstimate(flops=whole.size, bytes_accessed=whole.size, transcendentals=0),
    )(whole, middle, end)


def solution(mesh):
    def step(*arrays):
        m, v = arrays[6:9], arrays[9:12]
        *rest, factor = exchange(*arrays)
        new, gradients, far = rest[:3], rest[3:6], rest[10]

        mine = lax.ppermute(far, "dp", [(2, 0), (3, 1), (4, 6), (5, 7)])
        sets = list(zip(m, v, gradients, strict=True))
        whole, new_m, new_v = finish(new, sets, factor)
        mine, whole, new_m, new_v = lax.optimization_barrier((mine, whole, new_m, new_v))
        other = lax.ppermute(mine, "dp", [(0, 1), (1, 0), (6, 7), (7, 6)])
        gate, up, down = whole
        up, other = lax.optimization_barrier((fill(up, far, mine, 0), other))
        return (gate, fill(up, other, other, 1), down, *new_m, *new_v)

    all_of, cut = P(), P(None, "dp")
    return jax.shard_map(
        step,
        mesh=mesh,
        in_specs=(P(("rep", "dp")),) * 3 + (all_of,) * 3 + (cut,) * 6,
        out_specs=(P("rep"),) * 3 + (P("rep", "dp"),) * 6,
        check_vma=False,
    )
```
